256 devices in a mesh: tensor: 64 (over x_hi, y, z), dp: 4 (over x_lo, core).
Axes of the slice: x: 4 (x_hi: 2, x_lo: 2; x = x_hi * 2 + x_lo), y: 4, z: 8, core: 2. Of those that a mesh axis runs over, the one named last changes fastest.
Arguments:
- base_weight: bfloat16 [2, 2, 4096, 14336], P(None, None, 'tensor', 'dp'), may hold values from -0.25 to 0.25
- adapter_left: bfloat16 [2, 2, 4096, 16], P(None, None, 'tensor'), may hold values from -0.059814453 to 0.059814453
- adapter_right: bfloat16 [2, 2, 16, 14336], P(None, None, None, 'dp'), may hold values from -1.5 to 1.5
- magnitude: bfloat16 [2, 2, 14336], P(None, None, 'dp'), may hold values from 16 to 256
Outputs:
- merged_weight: bfloat16 [2, 2, 14336, 4096], P(None, None, 'tensor')
The draws below stay inside these ranges and needn't reach their ends.
All inputs are finite; a program needn't handle non-finite values.
Results may differ from the reference program's by a relative error of at most 0.0004.
Values may be sent and summed in bfloat16 or wider, within the bound.
A program may use at most 128 MiB of HBM per device.

```python
import math
import jax
import jax.numpy as jnp
from jax import lax

D = 4096
FF = 14336
RANK = 16
EXP = 2
PROJ = 2


def with_spikes(result, key, source, target, blocks, factor):
    def block_of(axis_at):
        return (jnp.arange(result.shape[axis_at]) // (result.shape[axis_at] // blocks)).reshape((-1,) + (1,) * (result.ndim - 1 - axis_at))

    first = jax.random.permutation(key, blocks)[block_of(target)]
    second = (block_of(target) + blocks // 2) % blocks
    return jnp.where((block_of(source) == first) | (block_of(source) == second), factor * result, result)


def block_scale(key, shape, pieces, low, high):
    def one(dim, parts):
        heights = jax.random.uniform(jax.random.fold_in(jax.random.fold_in(key, 6), dim), (parts,), jnp.float32, low / len(pieces), high / len(pieces))
        return jnp.repeat(jnp.exp(heights), shape[dim] // parts).reshape((-1,) + (1,) * (len(shape) - dim - 1))

    level = one(*pieces[0])
    for cut in pieces[1:]:
        level = level * one(*cut)
    return level


def noise(rng, extent, scale, bound, cuts=(), dtype=jnp.bfloat16):
    entries = scale * jax.random.normal(rng, extent, jnp.float32)
    if cuts:
        entries = entries * block_scale(rng, extent, cuts, -0.22, 0.18)
    return jnp.clip(entries, -bound, bound).astype(dtype)


def bell_draw_with(stream_key, extent, deviation, most, pieces, heavy, kind=jnp.bfloat16):
    drawn = deviation * jax.random.normal(stream_key, extent, jnp.float32)
    if pieces:
        drawn = drawn * block_scale(stream_key, extent, pieces, -0.22, 0.18)
    return jnp.clip(with_spikes(drawn, jax.random.fold_in(stream_key, 3), *heavy), -most, most).astype(kind)


def setup_inputs(seed: int = 0) -> dict:
    key_of = jax.random.split(jax.random.key(seed), 5)
    return {
        "base_weight": bell_draw_with(key_of[0], (EXP, PROJ, D, FF), D ** -0.5, 0.25, ((2, 64), (3, 4)), (2, 3, 64, 4.0)),
        "adapter_left": noise(key_of[1], (EXP, PROJ, D, RANK), 0.01, 0.059814453, ((2, 64),)),
        "adapter_right": noise(key_of[2], (EXP, PROJ, RANK, FF), RANK ** -0.5, 1.5, ((3, 4),)),
        "magnitude": jnp.clip(jnp.exp(math.log(256.0) - 2.7725887 * jax.random.uniform(key_of[3], (EXP, PROJ, FF), jnp.float32) ** block_scale(key_of[3], (EXP, PROJ, FF), ((2, 4),), -0.2, 0.2)), 16.0, 256.0).astype(jnp.bfloat16),
    }


def merge_one(operands):
    weight, left_factor, right_factor, column_scale = operands
    merged = weight.astype(jnp.float32) + jnp.dot(left_factor, right_factor, preferred_element_type=jnp.float32)
    squares = lax.optimization_barrier(jnp.sum(merged * merged, axis=0))
    scaling = column_scale.astype(jnp.float32) / jnp.sqrt(squares + 1e-06)
    return (merged * scaling[None, :]).astype(jnp.bfloat16).T

def reference(base_weight, adapter_left, adapter_right, magnitude):
    stacked = lax.map(merge_one, (base_weight.reshape(EXP * PROJ, D, FF), adapter_left.reshape(EXP * PROJ, D, RANK), adapter_right.reshape(EXP * PROJ, RANK, FF), magnitude.reshape(EXP * PROJ, FF)))
    return stacked.reshape(EXP, PROJ, FF, D)
```

```python
import functools

import jax
import jax.numpy as jnp
from jax import lax
from jax.experimental import pallas as pl
from jax.experimental.pallas import tpu as pltpu
from jax.sharding import PartitionSpec as P

MESH = pl.DeviceIdType.MESH
F32, BF16 = jnp.float32, jnp.bfloat16

T = 64
ROWS = 64
SERVE = 224
EPS = 4
TILES = 7
WROWS = TILES * ROWS
LROWS = 32
BROWS = WROWS + LROWS
RROWS = 32

DZ_EVEN = (4, 2, -2, 0)
DZ_ODD = (-3, -1, 3, 1)
DZ_SEND = (4, -3, 2, -1, -2, 3, 1, 0)


def packed(load, m):
    hole = 3 - m
    full = [load(e, 2 * m) for e in range(EPS)]
    rest = []
    for e in range(EPS):
        if m == 0:
            rest.append(load(e, 1))
        elif m == 3:
            rest.append(load(e, 5))
        else:
            low, high = load(e, 2 * m + 1), load(e, 2 * m - 1)
            group = lax.broadcasted_iota(jnp.int32, low.shape, 1) // 32
            rest.append(jnp.where(group < hole, low, high))
    last = rest[3]
    group = lax.broadcasted_iota(jnp.int32, last.shape, 1) // 32
    for k in range(3):
        full.append(jnp.where(group == hole, pltpu.roll(last, 32 * (k + 1), 1), rest[k]))
    return full


def comm_kernel(x_ref, l_ref, r_ref, m_ref, recv_ref, rm_ref, send_buf, rsend, a_send, f_send, r_send, recv_sem, r_recv):
    t, q = lax.axis_index("tensor"), lax.axis_index("dp")
    xh, y, z = t // 32, (t // 8) % 4, t % 8
    xl, c = q // 2, q % 2
    nbr, peer = q + 2 - 4 * xl, q + 1 - 2 * c

    src_q = xh * 2 + y // 2

    def direct(s):
        i, p, h = s // 4, (s // 2) % 2, s % 2
        odd = (z + c) % 2
        dz = jnp.where(odd == 1, DZ_ODD[i], DZ_EVEN[i])
        zs = (z - dz + 8) % 8
        ys = (y + p) % 2 + 2 * h
        return ys * 8 + zs

    barrier = pltpu.get_barrier_semaphore()
    self_in = 0
    for s in range(16):
        ts = xl * 32 + direct(s)
        same = jnp.logical_and(ts == t, src_q == q)
        self_in = self_in + same.astype(jnp.int32)

        @pl.when(jnp.logical_not(same))
        def _():
            pl.semaphore_signal(barrier, inc=1, device_id=(ts, src_q), device_id_type=MESH)

    for other in (nbr, peer, 3 - q):
        pl.semaphore_signal(barrier, inc=1, device_id=(t, other), device_id_type=MESH)

    lanes = lax.broadcasted_iota(jnp.int32, (16, 128), 1)
    ranks = lax.broadcasted_iota(jnp.int32, (16, 128), 0)
    lpack = jnp.zeros((LROWS, 128), F32)
    for half in range(2):
        for e in range(EPS):
            place = (lanes == half * 64 + e * 16 + ranks).astype(BF16)
            lpack += jnp.dot(l_ref[e, half * 32 : half * 32 + 32, :], place, preferred_element_type=F32)
    lpack = lpack.astype(BF16)

    @pl.loop(0, 4)
    def _(g):
        base = g * (TILES * 128)

        def at(k):
            return pl.ds(pl.multiple_of(base + 128 * k, 128), 128)

        for m in range(4):
            d = g * 4 + m
            for j, tile in enumerate(packed(lambda e, k: x_ref[e, :, at(k)].astype(F32), m)):
                send_buf[d, j * ROWS : (j + 1) * ROWS, :] = tile.astype(BF16)
            send_buf[d, WROWS:, :] = lpack
            rt = packed(lambda e, k: r_ref[e, :, at(k)].astype(F32), m)
            mt = packed(lambda e, k: m_ref[:, at(k)].astype(F32)[e : e + 1], m)
            for j in range(TILES):
                rows = jnp.concatenate([rt[j], jnp.broadcast_to(mt[j], (16, 128))], axis=0)
                rsend[d, j * RROWS : (j + 1) * RROWS, :] = rows.astype(BF16)

    self_out = jnp.logical_and(jnp.logical_and(xl == xh, y // 2 == c), z % 2 == c).astype(jnp.int32)
    pl.semaphore_wait(barrier, 19 - self_out)
    dst_q = xh * 2 + z % 2

    def block_copy(src, slot, send, dev):
        return pltpu.make_async_remote_copy(
            src_ref=src, dst_ref=recv_ref.at[slot], send_sem=send, recv_sem=recv_sem.at[slot], device_id=dev, device_id_type=MESH
        )

    def outgoing(k):
        dz, p = DZ_SEND[k // 2], k % 2
        yd, zd = (y + p) % 2, (z + dz + 8) % 8
        d = yd * 8 + zd
        td = 16 * q + d
        same = jnp.logical_and(td == t, dst_q == q)
        return d, td, same

    for k in range(16):
        d, td, same = outgoing(k)

        @pl.when(same)
        def _():
            pltpu.make_async_copy(send_buf.at[d], recv_ref.at[t], recv_sem.at[t]).start()

        @pl.when(jnp.logical_not(same))
        def _():
            block_copy(send_buf.at[d], t, a_send.at[k], (td, dst_q)).start()

    owner = t // 16
    mine = q == owner

    def r_copy(k):
        return pltpu.make_async_remote_copy(
            src_ref=rsend.at[t % 16], dst_ref=rm_ref, send_sem=r_send.at[k], recv_sem=r_recv, device_id=(t, (q + 1 + k) % 4), device_id_type=MESH
        )

    @pl.when(mine)
    def _():
        for k in range(3):
            r_copy(k).start()
        pltpu.make_async_copy(rsend.at[t % 16], rm_ref, r_recv).start()

    def arrived(slot):
        block_copy(recv_ref.at[slot], slot, f_send.at[0], (t, peer)).wait_recv()

    def forward(slot, k, other):
        block_copy(recv_ref.at[slot], slot, f_send.at[k], (t, other)).start()

    for s in range(17):
        if s < 16:
            slot = xl * 32 + direct(s)
            arrived(slot)
            forward(slot, s, nbr)
            forward(slot, 16 + s, peer)
        if s >= 1:
            slot = (1 - xl) * 32 + direct(s - 1)
            arrived(slot)
            forward(slot, 32 + s - 1, peer)

    @pl.loop(0, 32)
    def _(n):
        arrived(n * 2 + 1 - c)

    pltpu.make_async_copy(rsend.at[0], rm_ref, r_recv).wait()
    for k in range(16):
        d, td, same = outgoing(k)

        @pl.when(jnp.logical_not(same))
        def _():
            block_copy(send_buf.at[d], t, a_send.at[k], (td, dst_q)).wait_send()

    @pl.loop(0, 48)
    def _(k):
        block_copy(recv_ref.at[0], 0, f_send.at[k], (t, peer)).wait_send()

    @pl.when(mine)
    def _():
        for k in range(3):
            r_copy(k).wait_send()


def nt(a, b):
    return lax.dot_general(a, b, (((1,), (1,)), ((), ())), preferred_element_type=F32)


def merge_kernel(w_ref, rm_ref, out_ref, merged, acc, lhs):
    m = lax.axis_index("tensor") % 4
    hole = 3 - m
    lane = lax.broadcasted_iota(jnp.int32, (128, 128), 1)
    row = lax.broadcasted_iota(jnp.int32, (128, 128), 0)
    eye = (lane == row).astype(BF16)

    mags = []
    for j in range(TILES):
        r = rm_ref[j * RROWS : j * RROWS + 16, :].astype(F32)
        r8 = jnp.concatenate([r] * 8, axis=0)
        e_row = (row // 16) % 4
        e_lane = j if j < 4 else jnp.where(lane // 32 == hole, 3, j - 4)
        rbd = jnp.where(e_row == e_lane, r8, 0.0).astype(BF16)
        lhs[j, :, 0:128] = eye
        lhs[j, :, 128:256] = nt(eye, rbd).astype(BF16)
        mags.append(nt(eye, rm_ref[j * RROWS + 16 : j * RROWS + 32, :])[:, 0:1])

    acc[...] = jnp.zeros_like(acc)
    low = lax.broadcasted_iota(jnp.int32, (LROWS, 128), 1) < 64

    @pl.loop(0, 16)
    def _(n):
        parts = []
        for k in range(4):
            lb = w_ref[n * 4 + k, WROWS:, :].astype(F32)
            parts += [jnp.where(low, lb, 0.0), jnp.where(low, 0.0, lb)]
        lm = jnp.concatenate(parts, axis=0).astype(BF16)
        for j in range(TILES):
            w = jnp.concatenate([w_ref[n * 4 + k, j * ROWS : (j + 1) * ROWS, :] for k in range(4)], axis=0)
            rhs = jnp.concatenate([w, lm], axis=1)
            o = nt(lhs[j], rhs)
            merged[j * 128 : (j + 1) * 128, pl.ds(pl.multiple_of(n * 256, 256), 256)] = o
            o2 = o * o
            acc[j * 128 : (j + 1) * 128, :] += o2[:, :128] + o2[:, 128:]

    def column(g):
        return jnp.where(g > hole, 32 * (g - hole - 1), 128 + 32 * m + 32 * g)

    for j in range(TILES):
        squares = jnp.sum(acc[j * 128 : (j + 1) * 128, :], axis=1, keepdims=True)
        scale = mags[j] / jnp.sqrt(squares + 1e-6)
        for g in range(4):
            if j < 4:
                start = SERVE * j + 32 * m + 32 * g
            else:
                k = j - 4
                from3 = (hole - k - 1 + 4) % 4
                start = jnp.where(hole == g, SERVE * 3 + column(from3), SERVE * k + column(g))
            rows = slice(j * 128 + g * 32, j * 128 + g * 32 + 32)
            out_ref[pl.ds(pl.multiple_of(start, 32), 32), :] = (merged[rows, :] * scale[g * 32 : g * 32 + 32]).astype(BF16)


def shards(base_weight, adapter_left, adapter_right, magnitude):
    x = base_weight.reshape(EPS, ROWS, 3584)
    left = adapter_left.reshape(EPS, ROWS, 16)
    right = adapter_right.reshape(EPS, 16, 3584)
    mag = magnitude.reshape(EPS, 3584)
    vmem = pl.BlockSpec(memory_space=pltpu.VMEM)
    recv, rm = pl.pallas_call(
        comm_kernel,
        out_shape=(jax.ShapeDtypeStruct((T, BROWS, 128), BF16), jax.ShapeDtypeStruct((TILES * RROWS, 128), BF16)),
        in_specs=[vmem] * 4,
        out_specs=(vmem, vmem),
        scratch_shapes=[
            pltpu.VMEM((16, BROWS, 128), BF16),
            pltpu.VMEM((16, TILES * RROWS, 128), BF16),
            pltpu.SemaphoreType.DMA((16,)),
            pltpu.SemaphoreType.DMA((48,)),
            pltpu.SemaphoreType.DMA((3,)),
            pltpu.SemaphoreType.DMA((T,)),
            pltpu.SemaphoreType.DMA,
        ],
        compiler_params=pltpu.CompilerParams(collective_id=0, has_side_effects=True),
        name="exchange",
    )(x, left, right, mag)
    out = pl.pallas_call(
        merge_kernel,
        out_shape=jax.ShapeDtypeStruct((EPS * SERVE, T * ROWS), BF16),
        in_specs=[vmem] * 2,
        out_specs=vmem,
        scratch_shapes=[
            pltpu.VMEM((EPS * SERVE, T * ROWS), F32),
            pltpu.VMEM((EPS * SERVE, 128), F32),
            pltpu.VMEM((TILES, 128, 256), BF16),
        ],
        compiler_params=pltpu.CompilerParams(vmem_limit_bytes=60 * 2**20),
        name="merge",
    )(recv, rm)
    return out.reshape(2, 2, SERVE, T * ROWS)


def solution(mesh):
    in_specs = (
        P(None, None, "tensor", "dp"),
        P(None, None, "tensor", None),
        P(None, None, None, "dp"),
        P(None, None, "dp"),
    )
    out_specs = P(None, None, "tensor", None)
    return jax.shard_map(shards, mesh=mesh, in_specs=in_specs, out_specs=out_specs, check_vma=False)
```

```python
import functools

import jax
import jax.numpy as jnp
from jax import lax
from jax.experimental import pallas as pl
from jax.experimental.pallas import tpu as pltpu
from jax.sharding import PartitionSpec as P

MESH = pl.DeviceIdType.MESH
F32, BF16 = jnp.float32, jnp.bfloat16

T = 64
ROWS = 64
SERVE = 224
EPS = 4
TILES = 7
WROWS = TILES * ROWS
LROWS = 32
BROWS = WROWS + LROWS
RROWS = 32
LAG1, LAG2 = 2, 2


def packed(load, m):
    hole = 3 - m
    full = [load(e, 2 * m) for e in range(EPS)]
    rest = []
    for e in range(EPS):
        if m == 0:
            rest.append(load(e, 1))
        elif m == 3:
            rest.append(load(e, 5))
        else:
            low, high = load(e, 2 * m + 1), load(e, 2 * m - 1)
            group = lax.broadcasted_iota(jnp.int32, low.shape, 1) // 32
            rest.append(jnp.where(group < hole, low, high))
    last = rest[3]
    group = lax.broadcasted_iota(jnp.int32, last.shape, 1) // 32
    for k in range(3):
        full.append(jnp.where(group == hole, pltpu.roll(last, 32 * (k + 1), 1), rest[k]))
    return full


def nt(a, b):
    return lax.dot_general(a, b, (((1,), (1,)), ((), ())), preferred_element_type=F32)


def offset(i):
    far = (i + 1) // 2
    return jnp.where(i % 2 == 1, far, -far)


def exchange_kernel(
    x_ref, l_ref, r_ref, m_ref, merged, scale_ref, send_buf, rsend, recv, relay, rm, acc, lhs, a_send, l_send, f_send, r_send, recv_sem, l_recv, r_recv
):
    t, q = lax.axis_index("tensor"), lax.axis_index("dp")
    xh, y, z = t // 32, (t // 8) % 4, t % 8
    xl, c = q // 2, q % 2
    nbr, peer = q + 2 - 4 * xl, q + 1 - 2 * c
    edge, inner = xh == xl, xh != xl
    mirror = (xl * 32 + y * 8 + z, 2 * xh + c)
    src_core, dst_core = y // 2, y % 2
    row_m = t % 4
    hole = 3 - row_m

    def source(s, parity):
        return (parity + 2 * (s % 2)) * 8 + (z - offset(s // 2) + 8) % 8

    barrier = pltpu.get_barrier_semaphore()

    @pl.loop(0, 16)
    def _(s):
        yz = source(s, c)

        @pl.when(jnp.logical_or(yz != y * 8 + z, src_core != c))
        def _():
            pl.semaphore_signal(barrier, inc=1, device_id=(xh * 32 + yz, xl * 2 + src_core), device_id_type=MESH)

    for other in (nbr, peer, 3 - q):
        pl.semaphore_signal(barrier, inc=1, device_id=(t, other), device_id_type=MESH)

    @pl.when(inner)
    def _():
        pl.semaphore_signal(barrier, inc=1, device_id=mirror, device_id_type=MESH)

    lanes = lax.broadcasted_iota(jnp.int32, (16, 128), 1)
    ranks = lax.broadcasted_iota(jnp.int32, (16, 128), 0)
    lpack = jnp.zeros((LROWS, 128), F32)
    for e in range(EPS):
        low = (lanes == e * 16 + ranks).astype(BF16)
        high = (lanes == 64 + e * 16 + ranks).astype(BF16)
        tn = functools.partial(lax.dot_general, dimension_numbers=(((0,), (0,)), ((), ())), preferred_element_type=F32)
        lpack += tn(l_ref[e], low)[:LROWS] + tn(l_ref[e], high)[LROWS:]
    lpack = lpack.astype(BF16)

    @pl.loop(0, 4)
    def _(g):
        base = g * (TILES * 128)

        def at(k):
            return pl.ds(pl.multiple_of(base + 128 * k, 128), 128)

        for m in range(4):
            d = g * 4 + m
            for j, tile in enumerate(packed(lambda e, k: x_ref[e, :, at(k)].astype(F32), m)):
                send_buf[d, j * ROWS : (j + 1) * ROWS, :] = tile.astype(BF16)
            send_buf[d, WROWS:, :] = lpack
            rt = packed(lambda e, k: r_ref[e, :, at(k)].astype(F32), m)
            mt = packed(lambda e, k: m_ref[e // 2, :, at(k)].astype(F32)[e % 2 : e % 2 + 1], m)
            for j in range(TILES):
                rows = jnp.concatenate([rt[j], jnp.broadcast_to(mt[j], (16, 128))], axis=0)
                rsend[d, j * RROWS : (j + 1) * RROWS, :] = rows.astype(BF16)

    self_out = jnp.logical_and(src_core == c, dst_core == c).astype(jnp.int32)
    pl.semaphore_wait(barrier, 19 - self_out + inner.astype(jnp.int32))

    def copy(src, dst, send, recv_s, dev):
        return pltpu.make_async_remote_copy(
            src_ref=src, dst_ref=dst, send_sem=send, recv_sem=recv_s, device_id=dev, device_id_type=MESH
        )

    mine = q == t // 16

    def r_copy(k):
        return copy(rsend.at[t % 16], rm, r_send.at[k], r_recv, (t, (q + 1 + k) % 4))

    @pl.when(mine)
    def _():
        for k in range(3):
            r_copy(k).start()
        pltpu.make_async_copy(rsend.at[t % 16], rm, r_recv).start()

    def outgoing(k):
        yd, zd = 2 * c + (y + k % 2) % 2, (z + offset(k // 2) + 8) % 8
        away = jnp.logical_or(jnp.logical_or(yd != y, zd != z), dst_core != c)
        return yd, zd, away

    @pl.loop(0, 16)
    def _(k):
        yd, zd, away = outgoing(k)
        d = (yd - 2 * c) * 8 + zd
        s = 2 * (k // 2) + y // 2
        dev = (xh * 32 + yd * 8 + zd, xl * 2 + dst_core)
        block = send_buf.at[d]

        @pl.when(jnp.logical_and(away, edge))
        def _():
            copy(block, recv.at[t], a_send.at[k], recv_sem.at[t], dev).start()

        @pl.when(jnp.logical_and(away, inner))
        def _():
            copy(block, relay.at[s], a_send.at[k], l_recv.at[s], dev).start()

        @pl.when(jnp.logical_and(jnp.logical_not(away), edge))
        def _():
            pltpu.make_async_copy(block, recv.at[t], recv_sem.at[t]).start()

        @pl.when(jnp.logical_and(jnp.logical_not(away), inner))
        def _():
            pltpu.make_async_copy(block, relay.at[s], l_recv.at[s]).start()

    def arrived(slot):
        copy(recv.at[slot], recv.at[slot], f_send.at[0], recv_sem.at[slot], (t, peer)).wait_recv()

    def forward(slot, k, other):
        copy(recv.at[slot], recv.at[slot], f_send.at[k], recv_sem.at[slot], (t, other)).start()

    def relayed(s):
        slot = xh * 32 + source(s, c)
        return copy(relay.at[s], recv.at[slot], l_send.at[s], recv_sem.at[slot], mirror)

    lane = lax.broadcasted_iota(jnp.int32, (128, 128), 1)
    row = lax.broadcasted_iota(jnp.int32, (128, 128), 0)
    eye = (lane == row).astype(BF16)

    def build_lhs():
        pltpu.make_async_copy(rsend.at[0], rm, r_recv).wait()
        for j in range(TILES):
            r = rm[j * RROWS : j * RROWS + 16, :].astype(F32)
            r8 = jnp.concatenate([r] * 8, axis=0)
            e_lane = j if j < 4 else jnp.where(lane // 32 == hole, 3, j - 4)
            rbd = jnp.where((row // 16) % 4 == e_lane, r8, 0.0).astype(BF16)
            lhs[j, :, 0:128] = eye
            lhs[j, :, 128:256] = nt(eye, rbd).astype(BF16)

    def column(g):
        return jnp.where(g > hole, 32 * (g - hole - 1), 128 + 32 * row_m + 32 * g)

    def row_start(j, g):
        if j < 4:
            return pl.multiple_of(SERVE * j + 32 * row_m + 32 * g, 32)
        k = j - 4
        from3 = (hole - k - 1 + 4) % 4
        return pl.multiple_of(jnp.where(hole == g, SERVE * 3 + column(from3), SERVE * k + column(g)), 32)

    starts = [[row_start(j, g) for g in range(4)] for j in range(TILES)]
    low_half = lax.broadcasted_iota(jnp.int32, (LROWS, 128), 1) < 64

    def unit(w):
        stage, who = w // 4, w % 4
        half = jnp.where(who >= 2, 1 - xl, xl)
        parity = jnp.where(who % 2 == 1, 1 - c, c)
        odd = z % 2
        step = jnp.where(stage == 0, 0, jnp.where(stage == 1, -2, jnp.where(stage == 2, 2, 4)))
        zp = (z - odd + (1 - 2 * odd) * step + 8) % 8
        firsts = [half * 32 + (parity + 2 * h) * 8 + zp for h in range(2)]
        slots = [f + k for f in firsts for k in range(2)]
        parts = []
        for s in slots:
            lb = recv[s, WROWS:, :].astype(F32)
            parts += [jnp.where(low_half, lb, 0.0), jnp.where(low_half, 0.0, lb)]
        lm = jnp.concatenate(parts, axis=0).astype(BF16)
        for j in range(TILES):
            wt = jnp.concatenate([recv[s, j * ROWS : (j + 1) * ROWS, :] for s in slots], axis=0)
            o = nt(lhs[j], jnp.concatenate([wt, lm], axis=1))
            for h in range(2):
                cols = pl.ds(pl.multiple_of(firsts[h] * 64, 128), 128)
                if j < 4:
                    merged[pl.ds(starts[j][0], 128), cols] = o[:, 128 * h : 128 * h + 128]
                else:
                    for g in range(4):
                        merged[pl.ds(starts[j][g], 32), cols] = o[32 * g : 32 * g + 32, 128 * h : 128 * h + 128]
            o2 = o * o
            acc[j * 128 : (j + 1) * 128, :] += o2[:, :128] + o2[:, 128:]

    acc[...] = jnp.zeros_like(acc)

    @pl.loop(0, 21)
    def _(s):
        @pl.when(jnp.logical_and(s < 16, inner))
        def _():
            copy(relay.at[s], relay.at[s], l_send.at[0], l_recv.at[s], mirror).wait_recv()
            relayed(s).start()

        a = s - LAG1

        @pl.when(jnp.logical_and(a >= 0, a < 16))
        def _():
            slot = xl * 32 + source(a, c)
            arrived(slot)
            forward(slot, a, nbr)
            forward(slot, 16 + a, peer)

        b = s - LAG1 - LAG2

        @pl.when(jnp.logical_and(b >= 0, b < 16))
        def _():
            slot = (1 - xl) * 32 + source(b, c)
            arrived(slot)
            forward(slot, 32 + b, peer)

        @pl.when(jnp.logical_and(a >= 1, a < 17))
        def _():
            arrived(xl * 32 + source(a - 1, 1 - c))

        @pl.when(jnp.logical_and(b >= 1, b < 17))
        def _():
            arrived((1 - xl) * 32 + source(b - 1, 1 - c))

        @pl.when(s == 6)
        def _():
            build_lhs()

        @pl.when(s >= 7)
        def _():
            @pl.loop(0, jnp.where(jnp.logical_or(s == 17, s == 18), 2, 1))
            def _(v):
                unit(jnp.where(s <= 16, s - 7, jnp.where(s <= 18, s - 7 + 2 * v, s - 5)))

    for j in range(TILES):
        squares = jnp.sum(acc[j * 128 : (j + 1) * 128, :], axis=1, keepdims=True)
        mags = nt(eye, rm[j * RROWS + 16 : j * RROWS + 32, :])[:, 0:1]
        scale = jnp.broadcast_to(mags / jnp.sqrt(squares + 1e-6), (128, 128))
        for g in range(4):
            scale_ref[pl.ds(starts[j][g], 32), :] = scale[32 * g : 32 * g + 32]

    @pl.loop(0, 16)
    def _(k):
        @pl.when(outgoing(k)[2])
        def _():
            copy(send_buf.at[0], relay.at[0], a_send.at[k], l_recv.at[0], mirror).wait_send()

        @pl.when(inner)
        def _():
            relayed(k).wait_send()

    @pl.loop(0, 48)
    def _(k):
        copy(recv.at[0], recv.at[0], f_send.at[k], recv_sem.at[0], (t, peer)).wait_send()

    @pl.when(mine)
    def _():
        for k in range(3):
            r_copy(k).wait_send()


def scale_kernel(merged, scale, out_ref):
    rows = pl.ds(pl.multiple_of(pl.program_id(0) * 64, 64), 64)
    s = scale[rows, :]

    @pl.loop(0, T * ROWS // 512)
    def _(k):
        for n in range(4):
            cols = pl.ds(pl.multiple_of(k * 512 + n * 128, 128), 128)
            out_ref[:, cols] = (merged[rows, cols] * s).astype(BF16)


def shards(base_weight, adapter_left, adapter_right, magnitude):
    x = base_weight.reshape(EPS, ROWS, 3584)
    left = jnp.swapaxes(adapter_left, 2, 3).reshape(EPS, 16, ROWS)
    right = adapter_right.reshape(EPS, 16, 3584)
    vmem = pl.BlockSpec(memory_space=pltpu.VMEM)
    merged, scale = pl.pallas_call(
        exchange_kernel,
        out_shape=(pltpu.VMEM((EPS * SERVE, T * ROWS), F32), pltpu.VMEM((EPS * SERVE, 128), F32)),
        in_specs=[vmem] * 4,
        out_specs=(vmem, vmem),
        scratch_shapes=[
            pltpu.VMEM((16, BROWS, 128), BF16),
            pltpu.VMEM((16, TILES * RROWS, 128), BF16),
            pltpu.VMEM((T, BROWS, 128), BF16),
            pltpu.VMEM((16, BROWS, 128), BF16),
            pltpu.VMEM((TILES * RROWS, 128), BF16),
            pltpu.VMEM((EPS * SERVE, 128), F32),
            pltpu.VMEM((TILES, 128, 256), BF16),
            pltpu.SemaphoreType.DMA((16,)),
            pltpu.SemaphoreType.DMA((16,)),
            pltpu.SemaphoreType.DMA((48,)),
            pltpu.SemaphoreType.DMA((3,)),
            pltpu.SemaphoreType.DMA((T,)),
            pltpu.SemaphoreType.DMA((16,)),
            pltpu.SemaphoreType.DMA,
        ],
        compiler_params=pltpu.CompilerParams(collective_id=0, has_side_effects=True, vmem_limit_bytes=24 * 2**20),
        name="exchange",
    )(x, left, right, magnitude)
    out = pl.pallas_call(
        scale_kernel,
        out_shape=jax.ShapeDtypeStruct((EPS * SERVE, T * ROWS), BF16),
        grid=(EPS * SERVE // 64,),
        in_specs=[vmem, vmem],
        out_specs=pl.BlockSpec((64, T * ROWS), lambda i: (i, 0)),
        compiler_params=pltpu.CompilerParams(vmem_limit_bytes=16 * 2**20),
        name="scale",
    )(merged, scale)
    return out.reshape(2, 2, SERVE, T * ROWS)


def solution(mesh):
    in_specs = (
        P(None, None, "tensor", "dp"),
        P(None, None, "tensor", None),
        P(None, None, None, "dp"),
        P(None, None, "dp"),
    )
    out_specs = P(None, None, "tensor", None)
    return jax.shard_map(shards, mesh=mesh, in_specs=in_specs, out_specs=out_specs, check_vma=False)
```

```python
import functools

import jax
import jax.numpy as jnp
from jax import lax
from jax.experimental import pallas as pl
from jax.experimental.pallas import tpu as pltpu
from jax.sharding import PartitionSpec as P

MESH = pl.DeviceIdType.MESH
F32, BF16 = jnp.float32, jnp.bfloat16

T = 64
ROWS = 64
SERVE = 224
EPS = 4
TILES = 7
WROWS = TILES * ROWS
LROWS = 32
BROWS = WROWS + LROWS
RROWS = 32
LAG1, LAG2, PLAG = 2, 2, 3


def packed(load, m):
    hole = 3 - m
    full = [load(e, 2 * m) for e in range(EPS)]
    rest = []
    for e in range(EPS):
        if m == 0:
            rest.append(load(e, 1))
        elif m == 3:
            rest.append(load(e, 5))
        else:
            low, high = load(e, 2 * m + 1), load(e, 2 * m - 1)
            group = lax.broadcasted_iota(jnp.int32, low.shape, 1) // 32
            rest.append(jnp.where(group < hole, low, high))
    last = rest[3].astype(F32)
    group = lax.broadcasted_iota(jnp.int32, last.shape, 1) // 32
    for k in range(3):
        full.append(jnp.where(group == hole, pltpu.roll(last, 32 * (k + 1), 1).astype(BF16), rest[k]))
    return full


def nt(a, b):
    return lax.dot_general(a, b, (((1,), (1,)), ((), ())), preferred_element_type=F32)


SENDS = tuple((d, p) for p in (0, 1) for d in (0, 1, -1, 2, -2)) + tuple((d, p) for p in (0, 1) for d in (3, -3, 4))


def arrival(s):
    far = 2 + (s - 6) // 4
    dz_near = jnp.where(s % 5 == 0, 0, jnp.where(s % 2 == 1, 1, -1))
    dz_far = jnp.where(s >= 14, 4, jnp.where(s % 2 == 0, far, -far))
    other = jnp.where(s < 6, s // 3, jnp.where(s < 14, (s - 6) // 2 % 2, s - 14))
    return jnp.where(s < 6, dz_near, dz_far), other


def exchange_kernel(
    x_hbm, l_hbm, r_hbm, m_hbm, merged, scale_ref, x_ref, l_ref, r_ref, m_ref, in_sem, send_buf, rsend, recv, relay, rm, acc, lhs, a_send, l_send, f_send, r_send, recv_sem, l_recv, r_recv
):
    t, q = lax.axis_index("tensor"), lax.axis_index("dp")
    xh, y, z = t // 32, (t // 8) % 4, t % 8
    xl, c = q // 2, q % 2
    nbr, peer = q + 2 - 4 * xl, q + 1 - 2 * c
    edge, inner = xh == xl, xh != xl
    mirror = (xl * 32 + y * 8 + z, 2 * xh + c)
    src_core, dst_core = y // 2, y % 2
    row_m = t % 4
    hole = 3 - row_m

    def source(s, parity):
        dz, other = arrival(s)
        return (y + (y + parity) % 2 + 2 * other) % 4 * 8 + (z - dz + 8) % 8

    def place(yz):
        return yz // 16 * 8 + yz % 8

    small_in = [pltpu.make_async_copy(a, b, in_sem.at[4 + k]) for k, (a, b) in enumerate(((l_hbm, l_ref), (r_hbm, r_ref), (m_hbm, m_ref)))]

    def x_in(g):
        cols = pl.ds(pl.multiple_of(g * (TILES * 128), 128), TILES * 128)
        return pltpu.make_async_copy(x_hbm.at[:, :, cols], x_ref.at[:, :, cols], in_sem.at[g])

    for a in small_in:
        a.start()
    for g in range(4):
        x_in(g).start()

    barrier = pltpu.get_barrier_semaphore()

    @pl.loop(0, 16)
    def _(s):
        yz = source(s, c)

        @pl.when(jnp.logical_or(yz != y * 8 + z, src_core != c))
        def _():
            pl.semaphore_signal(barrier, inc=1, device_id=(xh * 32 + yz, xl * 2 + src_core), device_id_type=MESH)

    for other in (nbr, peer, 3 - q):
        pl.semaphore_signal(barrier, inc=1, device_id=(t, other), device_id_type=MESH)

    @pl.when(inner)
    def _():
        pl.semaphore_signal(barrier, inc=1, device_id=mirror, device_id_type=MESH)

    for a in small_in:
        a.wait()
    lanes = lax.broadcasted_iota(jnp.int32, (16, 128), 1)
    ranks = lax.broadcasted_iota(jnp.int32, (16, 128), 0)
    lpack = jnp.zeros((LROWS, 128), F32)
    for e in range(EPS):
        low = (lanes == e * 16 + ranks).astype(BF16)
        high = (lanes == 64 + e * 16 + ranks).astype(BF16)
        tn = functools.partial(lax.dot_general, dimension_numbers=(((0,), (0,)), ((), ())), preferred_element_type=F32)
        lpack += tn(l_ref[e], low)[:LROWS] + tn(l_ref[e], high)[LROWS:]
    lpack = lpack.astype(BF16)

    @pl.loop(0, 4)
    def _(g):
        base = g * (TILES * 128)
        x_in(g).wait()

        def at(k):
            return pl.ds(pl.multiple_of(base + 128 * k, 128), 128)

        for m in range(4):
            d = g * 4 + m
            for j, tile in enumerate(packed(lambda e, k: x_ref[e, :, at(k)], m)):
                send_buf[d, j * ROWS : (j + 1) * ROWS, :] = tile
            send_buf[d, WROWS:, :] = lpack

    mine = q == t // 16
    for m in range(4):

        @pl.when(jnp.logical_and(mine, row_m == m))
        def _():
            base = t % 16 // 4 * (TILES * 128)

            def at(k):
                return pl.ds(pl.multiple_of(base + 128 * k, 128), 128)

            rt = packed(lambda e, k: r_ref[e, :, at(k)], m)
            mt = packed(lambda e, k: jnp.broadcast_to(m_ref[e // 2, :, at(k)].astype(F32)[e % 2 : e % 2 + 1], (16, 128)).astype(BF16), m)
            for j in range(TILES):
                rsend[j * RROWS : j * RROWS + 16, :] = rt[j]
                rsend[j * RROWS + 16 : (j + 1) * RROWS, :] = mt[j]

    self_out = jnp.logical_and(src_core == c, dst_core == c).astype(jnp.int32)
    pl.semaphore_wait(barrier, 19 - self_out + inner.astype(jnp.int32))

    def copy(src, dst, send, recv_s, dev):
        return pltpu.make_async_remote_copy(
            src_ref=src, dst_ref=dst, send_sem=send, recv_sem=recv_s, device_id=dev, device_id_type=MESH
        )

    def r_copy(k):
        return copy(rsend, rm, r_send.at[k], r_recv, (t, (q + 1 + k) % 4))

    @pl.when(mine)
    def _():
        for k in range(3):
            r_copy(k).start()
        pltpu.make_async_copy(rsend, rm, r_recv).start()

    def outgoing(k):
        dz, p = SENDS[k]
        yd, zd = 2 * c + (y + p) % 2, (z + dz + 8) % 8
        away = jnp.logical_or(jnp.logical_or(yd != y, zd != z), dst_core != c)
        return yd, zd, away

    own = place(y * 8 + z)
    for k in range(16):
        yd, zd, away = outgoing(k)
        dev = (xh * 32 + yd * 8 + zd, xl * 2 + dst_core)
        block = send_buf.at[(yd - 2 * c) * 8 + zd]

        @pl.when(jnp.logical_and(away, edge))
        def _():
            copy(block, recv.at[t], a_send.at[k], recv_sem.at[t], dev).start()

        @pl.when(jnp.logical_and(away, inner))
        def _():
            copy(block, relay.at[own], a_send.at[k], l_recv.at[own], dev).start()

        @pl.when(jnp.logical_and(jnp.logical_not(away), edge))
        def _():
            pltpu.make_async_copy(block, recv.at[t], recv_sem.at[t]).start()

        @pl.when(jnp.logical_and(jnp.logical_not(away), inner))
        def _():
            pltpu.make_async_copy(block, relay.at[own], l_recv.at[own]).start()

    def arrived(slot):
        copy(recv.at[slot], recv.at[slot], f_send.at[0], recv_sem.at[slot], (t, peer)).wait_recv()

    def forward(slot, k, other):
        copy(recv.at[slot], recv.at[slot], f_send.at[k], recv_sem.at[slot], (t, other)).start()

    def relayed(s):
        yz = source(s, c)
        slot = xh * 32 + yz
        return copy(relay.at[place(yz)], recv.at[slot], l_send.at[s], recv_sem.at[slot], mirror)

    lane = lax.broadcasted_iota(jnp.int32, (128, 128), 1)
    row = lax.broadcasted_iota(jnp.int32, (128, 128), 0)
    eye = (lane == row).astype(BF16)

    def build_lhs():
        pltpu.make_async_copy(rsend, rm, r_recv).wait()
        for j in range(TILES):
            r = rm[j * RROWS : j * RROWS + 16, :].astype(F32)
            r8 = jnp.concatenate([r] * 8, axis=0)
            e_lane = j if j < 4 else jnp.where(lane // 32 == hole, 3, j - 4)
            rbd = jnp.where((row // 16) % 4 == e_lane, r8, 0.0).astype(BF16)
            lhs[j, :, 0:128] = eye
            lhs[j, :, 128:256] = nt(eye, rbd).astype(BF16)

    def column(g):
        return jnp.where(g > hole, 32 * (g - hole - 1), 128 + 32 * row_m + 32 * g)

    def row_start(j, g):
        if j < 4:
            return pl.multiple_of(SERVE * j + 32 * row_m + 32 * g, 32)
        k = j - 4
        from3 = (hole - k - 1 + 4) % 4
        return pl.multiple_of(jnp.where(hole == g, SERVE * 3 + column(from3), SERVE * k + column(g)), 32)

    starts = [[row_start(j, g) for g in range(4)] for j in range(TILES)]
    low_half = lax.broadcasted_iota(jnp.int32, (LROWS, 128), 1) < 64

    def unit(w):
        stage, who = w // 4, w % 4
        half = jnp.where(who % 2 == 1, 1 - xl, xl)
        parity = jnp.where(who >= 2, 1 - c, c)
        odd = z % 2
        step = jnp.where(stage == 0, 0, jnp.where(stage == 1, -2, jnp.where(stage == 2, 2, 4)))
        zp = (z - odd + (1 - 2 * odd) * step + 8) % 8
        firsts = [half * 32 + (parity + 2 * h) * 8 + zp for h in range(2)]
        slots = [f + k for f in firsts for k in range(2)]
        parts = []
        for s in slots:
            lb = recv[s, WROWS:, :].astype(F32)
            parts += [jnp.where(low_half, lb, 0.0), jnp.where(low_half, 0.0, lb)]
        lm = jnp.concatenate(parts, axis=0).astype(BF16)
        for j in range(TILES):
            wt = jnp.concatenate([recv[s, j * ROWS : (j + 1) * ROWS, :] for s in slots], axis=0)
            o = nt(lhs[j], jnp.concatenate([wt, lm], axis=1))
            for h in range(2):
                cols = pl.ds(pl.multiple_of(firsts[h] * 64, 128), 128)
                if j < 4:
                    merged[pl.ds(starts[j][0], 128), cols] = o[:, 128 * h : 128 * h + 128]
                else:
                    for g in range(4):
                        merged[pl.ds(starts[j][g], 32), cols] = o[32 * g : 32 * g + 32, 128 * h : 128 * h + 128]
            o2 = o * o
            acc[j * 128 : (j + 1) * 128, :] += o2[:, :128] + o2[:, 128:]

    acc[...] = jnp.zeros_like(acc)

    @pl.loop(0, 23)
    def _(s):
        @pl.when(jnp.logical_and(s < 16, inner))
        def _():
            here = place(source(s, c))
            copy(relay.at[here], relay.at[here], l_send.at[0], l_recv.at[here], mirror).wait_recv()
            relayed(s).start()

        a = s - LAG1

        @pl.when(jnp.logical_and(a >= 0, a < 16))
        def _():
            slot = xl * 32 + source(a, c)
            arrived(slot)
            forward(slot, a, nbr)
            forward(slot, 16 + a, peer)

        b = s - LAG1 - LAG2

        @pl.when(jnp.logical_and(b >= 0, b < 16))
        def _():
            slot = (1 - xl) * 32 + source(b, c)
            arrived(slot)
            forward(slot, 32 + b, peer)

        @pl.when(jnp.logical_and(a >= PLAG, a < 16 + PLAG))
        def _():
            arrived(xl * 32 + source(a - PLAG, 1 - c))

        @pl.when(jnp.logical_and(b >= PLAG, b < 16 + PLAG))
        def _():
            arrived((1 - xl) * 32 + source(b - PLAG, 1 - c))

        @pl.when(s == 6)
        def _():
            build_lhs()

        @pl.when(s >= 9)
        def _():
            @pl.loop(0, jnp.where(jnp.logical_or(s == 18, s == 20), 2, 1))
            def _(v):
                unit(jnp.where(s <= 19, s - 9 + 3 * v, jnp.where(s == 20, 11 + 2 * v, s - 7)))

    for j in range(TILES):
        squares = jnp.sum(acc[j * 128 : (j + 1) * 128, :], axis=1, keepdims=True)
        mags = nt(eye, rm[j * RROWS + 16 : j * RROWS + 32, :])[:, 0:1]
        scale = jnp.broadcast_to(mags / jnp.sqrt(squares + 1e-6), (128, 128))
        for g in range(4):
            scale_ref[pl.ds(starts[j][g], 32), :] = scale[32 * g : 32 * g + 32]

    for k in range(16):

        @pl.when(outgoing(k)[2])
        def _():
            copy(send_buf.at[0], relay.at[0], a_send.at[k], l_recv.at[0], mirror).wait_send()

    @pl.loop(0, 16)
    def _(k):
        @pl.when(inner)
        def _():
            relayed(k).wait_send()

    @pl.loop(0, 48)
    def _(k):
        copy(recv.at[0], recv.at[0], f_send.at[k], recv_sem.at[0], (t, peer)).wait_send()

    @pl.when(mine)
    def _():
        for k in range(3):
            r_copy(k).wait_send()


def scale_kernel(merged, scale, out_hbm, out_ref, sems):
    def written(k):
        rows = pl.ds(k * 128, 128)
        return pltpu.make_async_copy(out_ref.at[rows], out_hbm.at[rows], sems.at[k])

    for k in range(TILES):

        @pl.loop(0, 8)
        def _(n):
            rows = pl.ds(pl.multiple_of(k * 128 + n * 16, 16), 16)
            s = scale[rows, :]
            for i in range(T * ROWS // 128):
                cols = slice(i * 128, i * 128 + 128)
                out_ref[rows, cols] = (merged[rows, cols] * s).astype(BF16)

        written(k).start()
    for k in range(TILES):
        written(k).wait()


def shards(base_weight, adapter_left, adapter_right, magnitude):
    x = base_weight.reshape(EPS, ROWS, 3584)
    left = jnp.swapaxes(adapter_left, 2, 3).reshape(EPS, 16, ROWS)
    right = adapter_right.reshape(EPS, 16, 3584)
    x, left, right, magnitude = (pltpu.with_memory_space_constraint(a, pltpu.HBM) for a in (x, left, right, magnitude))
    vmem = pl.BlockSpec(memory_space=pltpu.VMEM)
    merged, scale = pl.pallas_call(
        exchange_kernel,
        out_shape=(pltpu.VMEM((EPS * SERVE, T * ROWS), F32), pltpu.VMEM((EPS * SERVE, 128), F32)),
        in_specs=[pl.BlockSpec(memory_space=pltpu.HBM)] * 4,
        out_specs=(vmem, vmem),
        scratch_shapes=[
            pltpu.VMEM((EPS, ROWS, 3584), BF16),
            pltpu.VMEM((EPS, 16, ROWS), BF16),
            pltpu.VMEM((EPS, 16, 3584), BF16),
            pltpu.VMEM((2, 2, 3584), BF16),
            pltpu.SemaphoreType.DMA((7,)),
            pltpu.VMEM((16, BROWS, 128), BF16),
            pltpu.VMEM((TILES * RROWS, 128), BF16),
            pltpu.VMEM((T, BROWS, 128), BF16),
            pltpu.VMEM((16, BROWS, 128), BF16),
            pltpu.VMEM((TILES * RROWS, 128), BF16),
            pltpu.VMEM((EPS * SERVE, 128), F32),
            pltpu.VMEM((TILES, 128, 256), BF16),
            pltpu.SemaphoreType.DMA((16,)),
            pltpu.SemaphoreType.DMA((16,)),
            pltpu.SemaphoreType.DMA((48,)),
            pltpu.SemaphoreType.DMA((3,)),
            pltpu.SemaphoreType.DMA((T,)),
            pltpu.SemaphoreType.DMA((16,)),
            pltpu.SemaphoreType.DMA,
        ],
        compiler_params=pltpu.CompilerParams(collective_id=0, has_side_effects=True, vmem_limit_bytes=24 * 2**20),
        name="exchange",
    )(x, left, right, magnitude)
    out = pl.pallas_call(
        scale_kernel,
        out_shape=jax.ShapeDtypeStruct((EPS * SERVE, T * ROWS), BF16),
        in_specs=[vmem, vmem],
        out_specs=pl.BlockSpec(memory_space=pltpu.HBM),
        scratch_shapes=[pltpu.VMEM((EPS * SERVE, T * ROWS), BF16), pltpu.SemaphoreType.DMA((TILES,))],
        compiler_params=pltpu.CompilerParams(vmem_limit_bytes=16 * 2**20),
        name="scale",
    )(merged, scale)
    return out.reshape(2, 2, SERVE, T * ROWS)


def solution(mesh):
    in_specs = (
        P(None, None, "tensor", "dp"),
        P(None, None, "tensor", None),
        P(None, None, None, "dp"),
        P(None, None, "dp"),
    )
    out_specs = P(None, None, "tensor", None)
    return jax.shard_map(shards, mesh=mesh, in_specs=in_specs, out_specs=out_specs, check_vma=False)
```

```python
import functools

import jax
import jax.numpy as jnp
from jax import lax
from jax.experimental import pallas as pl
from jax.experimental.pallas import tpu as pltpu
from jax.sharding import PartitionSpec as P

MESH = pl.DeviceIdType.MESH
F32, BF16 = jnp.float32, jnp.bfloat16

T = 64
ROWS = 64
SERVE = 224
EPS = 4
TILES = 7
WROWS = TILES * ROWS
LROWS = 32
BROWS = WROWS + LROWS
RROWS = TILES * 16 + 16
LAG1, LAG2 = 2, 2
FIRST = 9
UNITS = (0, 1, 4, 2, 5, 3, 8, 6, 9, 12, 10, 13, 14, 15)


def packed(load, m):
    hole = 3 - m
    full = [load(e, 2 * m) for e in range(EPS)]
    rest = []
    for e in range(EPS):
        if m == 0:
            rest.append(load(e, 1))
        elif m == 3:
            rest.append(load(e, 5))
        else:
            low, high = load(e, 2 * m + 1), load(e, 2 * m - 1)
            group = lax.broadcasted_iota(jnp.int32, low.shape, 1) // 32
            rest.append(jnp.where(group < hole, low, high))
    last = rest[3].astype(F32)
    group = lax.broadcasted_iota(jnp.int32, last.shape, 1) // 32
    for k in range(3):
        full.append(jnp.where(group == hole, pltpu.roll(last, 32 * (k + 1), 1).astype(BF16), rest[k]))
    return full


def nt(a, b):
    return lax.dot_general(a, b, (((1,), (1,)), ((), ())), preferred_element_type=F32)


SENDS = tuple((d, p) for d in (0, 1, -1, 2, -2, 3, -3, 4) for p in (0, 1))


def arrival(s):
    even = lax.rem(s, 2) == 0
    far = jnp.where(s >= 10, 3, 2)
    dz_near = jnp.where(jnp.logical_or(s == 0, s == 5), 0, jnp.where(even, -1, 1))
    dz_far = jnp.where(s >= 14, 4, jnp.where(even, far, -far))
    late = jnp.where(s < 6, s >= 3, jnp.where(s < 10, s >= 8, jnp.where(s < 14, s >= 12, s == 15)))
    return jnp.where(s < 6, dz_near, dz_far), late


def exchange_kernel(
    x_hbm, l_hbm, r_hbm, m_hbm, merged, scale_ref, x_ref, l_ref, r_ref, m_ref, in_sem, send_buf, rsend, recv, relay, rm, acc, lhs, a_send, l_send, f_send, r_send, recv_sem, l_recv, r_recv
):
    t, q = lax.axis_index("tensor"), lax.axis_index("dp")
    xh, y, z = t // 32, (t // 8) % 4, t % 8
    xl, c = q // 2, q % 2
    nbr, peer = q + 2 - 4 * xl, q + 1 - 2 * c
    edge, inner = xh == xl, xh != xl
    mirror = (xl * 32 + y * 8 + z, 2 * xh + c)
    src_core, dst_core = y // 2, y % 2
    row_m = t % 4
    hole = 3 - row_m

    y_rows = [[(y + (y + parity) % 2 + 2 * w) % 4 * 8 for w in range(2)] for parity in (c, 1 - c)]

    def source(s, who):
        dz, late = arrival(s)
        return jnp.where(late, y_rows[who][1], y_rows[who][0]) + lax.rem(z - dz + 8, 8)

    def place(yz):
        return lax.div(yz, 16) * 8 + lax.rem(yz, 8)

    small_in = [pltpu.make_async_copy(a, b, in_sem.at[4 + k]) for k, (a, b) in enumerate(((l_hbm, l_ref), (r_hbm, r_ref), (m_hbm, m_ref)))]

    def x_in(g):
        cols = pl.ds(pl.multiple_of(g * (TILES * 128), 128), TILES * 128)
        return pltpu.make_async_copy(x_hbm.at[:, :, cols], x_ref.at[:, :, cols], in_sem.at[g])

    for a in small_in:
        a.start()
    for g in range(4):
        x_in(g).start()

    barrier = pltpu.get_barrier_semaphore()

    @pl.loop(0, 16)
    def _(s):
        yz = source(s, 0)

        @pl.when(jnp.logical_or(yz != y * 8 + z, src_core != c))
        def _():
            pl.semaphore_signal(barrier, inc=1, device_id=(xh * 32 + yz, xl * 2 + src_core), device_id_type=MESH)

    for other in (nbr, peer):
        pl.semaphore_signal(barrier, inc=1, device_id=(t, other), device_id_type=MESH)

    @pl.when(inner)
    def _():
        pl.semaphore_signal(barrier, inc=1, device_id=mirror, device_id_type=MESH)

    for a in small_in:
        a.wait()
    lanes = lax.broadcasted_iota(jnp.int32, (16, 128), 1)
    ranks = lax.broadcasted_iota(jnp.int32, (16, 128), 0)
    lpack = jnp.zeros((LROWS, 128), F32)
    for e in range(EPS):
        low = (lanes == e * 16 + ranks).astype(BF16)
        high = (lanes == 64 + e * 16 + ranks).astype(BF16)
        tn = functools.partial(lax.dot_general, dimension_numbers=(((0,), (0,)), ((), ())), preferred_element_type=F32)
        lpack += tn(l_ref[e], low)[:LROWS] + tn(l_ref[e], high)[LROWS:]
    lpack = lpack.astype(BF16)

    @pl.loop(0, 4)
    def _(g):
        base = g * (TILES * 128)
        x_in(g).wait()

        def at(k):
            return pl.ds(pl.multiple_of(base + 128 * k, 128), 128)

        for m in range(4):
            d = g * 4 + m
            for j, tile in enumerate(packed(lambda e, k: x_ref[e, :, at(k)], m)):
                send_buf[d, j * ROWS : (j + 1) * ROWS, :] = tile
            send_buf[d, WROWS:, :] = lpack

    mine = q == t // 16
    for m in range(4):

        @pl.when(jnp.logical_and(mine, row_m == m))
        def _():
            base = t % 16 // 4 * (TILES * 128)

            def at(k):
                return pl.ds(pl.multiple_of(base + 128 * k, 128), 128)

            rt = packed(lambda e, k: r_ref[e, :, at(k)], m)
            mt = packed(lambda e, k: jnp.broadcast_to(m_ref[e // 2, :, at(k)].astype(F32)[e % 2 : e % 2 + 1], (16, 128)).astype(BF16), m)
            mags = jnp.zeros((16, 128), F32)
            for j in range(TILES):
                rsend[j * 16 : j * 16 + 16, :] = rt[j]
                mags = jnp.where(ranks == j, mt[j].astype(F32), mags)
            rsend[TILES * 16 :, :] = mags.astype(BF16)

    self_out = jnp.logical_and(src_core == c, dst_core == c).astype(jnp.int32)
    pl.semaphore_wait(barrier, 18 - self_out + inner.astype(jnp.int32))

    def copy(src, dst, send, recv_s, dev):
        return pltpu.make_async_remote_copy(
            src_ref=src, dst_ref=dst, send_sem=send, recv_sem=recv_s, device_id=dev, device_id_type=MESH
        )

    second = nbr == t // 16

    def r_copy(src, k):
        return copy(src, rm, r_send.at[k], r_recv, (t, (peer, nbr)[k]))

    @pl.when(mine)
    def _():
        for k in range(2):
            r_copy(rsend, k).start()
        pltpu.make_async_copy(rsend, rm, r_recv).start()

    def outgoing(k):
        dz, p = SENDS[k]
        yd, zd = 2 * c + (y + p) % 2, (z + dz + 8) % 8
        away = jnp.logical_or(jnp.logical_or(yd != y, zd != z), dst_core != c)
        return yd, zd, away

    own = place(y * 8 + z)
    for k in range(16):
        yd, zd, away = outgoing(k)
        dev = (xh * 32 + yd * 8 + zd, xl * 2 + dst_core)
        block = send_buf.at[(yd - 2 * c) * 8 + zd]

        @pl.when(jnp.logical_and(away, edge))
        def _():
            copy(block, recv.at[t], a_send.at[k], recv_sem.at[t], dev).start()

        @pl.when(jnp.logical_and(away, inner))
        def _():
            copy(block, relay.at[own], a_send.at[k], l_recv.at[own], dev).start()

        @pl.when(jnp.logical_and(jnp.logical_not(away), edge))
        def _():
            pltpu.make_async_copy(block, recv.at[t], recv_sem.at[t]).start()

        @pl.when(jnp.logical_and(jnp.logical_not(away), inner))
        def _():
            pltpu.make_async_copy(block, relay.at[own], l_recv.at[own]).start()

    def arrived(slot):
        copy(recv.at[slot], recv.at[slot], f_send.at[0], recv_sem.at[slot], (t, peer)).wait_recv()

    def forward(slot, k, other):
        copy(recv.at[slot], recv.at[slot], f_send.at[k], recv_sem.at[slot], (t, other)).start()

    def relayed(s):
        yz = source(s, 0)
        slot = xh * 32 + yz
        return copy(relay.at[place(yz)], recv.at[slot], l_send.at[s], recv_sem.at[slot], mirror)

    lane = lax.broadcasted_iota(jnp.int32, (128, 128), 1)
    row = lax.broadcasted_iota(jnp.int32, (128, 128), 0)
    eye = (lane == row).astype(BF16)

    def build_lhs():
        for j in range(TILES):
            r = rm[j * 16 : j * 16 + 16, :].astype(F32)
            r8 = jnp.concatenate([r] * 8, axis=0)
            e_lane = j if j < 4 else jnp.where(lane // 32 == hole, 3, j - 4)
            rbd = jnp.where((row // 16) % 4 == e_lane, r8, 0.0).astype(BF16)
            lhs[j, :, 0:128] = eye
            lhs[j, :, 128:256] = nt(eye, rbd).astype(BF16)

    def column(g):
        return jnp.where(g > hole, 32 * (g - hole - 1), 128 + 32 * row_m + 32 * g)

    def row_start(j, g):
        if j < 4:
            return pl.multiple_of(SERVE * j + 32 * row_m + 32 * g, 32)
        k = j - 4
        from3 = (hole - k - 1 + 4) % 4
        return pl.multiple_of(jnp.where(hole == g, SERVE * 3 + column(from3), SERVE * k + column(g)), 32)

    starts = [[row_start(j, g) for g in range(4)] for j in range(TILES)]
    low_half = lax.broadcasted_iota(jnp.int32, (LROWS, 128), 1) < 64

    def unit(w):
        stage, who = w // 4, w % 4
        half = jnp.where(who % 2 == 1, 1 - xl, xl)
        parity = jnp.where(who >= 2, 1 - c, c)
        odd = z % 2
        step = jnp.where(stage == 0, 0, jnp.where(stage == 1, -2, jnp.where(stage == 2, 2, 4)))
        zp = (z - odd + (1 - 2 * odd) * step + 8) % 8
        firsts = [half * 32 + (parity + 2 * h) * 8 + zp for h in range(2)]
        slots = [f + k for f in firsts for k in range(2)]

        @pl.when(who >= 2)
        def _():
            @pl.loop(jnp.where(stage == 0, 0, 2 + 4 * stage), jnp.where(stage == 3, 16, 6 + 4 * stage))
            def _(i):
                arrived(half * 32 + source(i, 1))

        parts = []
        for s in slots:
            lb = recv[s, WROWS:, :].astype(F32)
            parts += [jnp.where(low_half, lb, 0.0), jnp.where(low_half, 0.0, lb)]
        lm = jnp.concatenate(parts, axis=0).astype(BF16)
        for j in range(TILES):
            wt = jnp.concatenate([recv[s, j * ROWS : (j + 1) * ROWS, :] for s in slots], axis=0)
            o = nt(lhs[j], jnp.concatenate([wt, lm], axis=1))
            for h in range(2):
                cols = pl.ds(pl.multiple_of(firsts[h] * 64, 128), 128)
                if j < 4:
                    merged[pl.ds(starts[j][0], 128), cols] = o[:, 128 * h : 128 * h + 128]
                else:
                    for g in range(4):
                        merged[pl.ds(starts[j][g], 32), cols] = o[32 * g : 32 * g + 32, 128 * h : 128 * h + 128]
            o2 = o * o
            acc[j * 128 : (j + 1) * 128, :] += o2[:, :128] + o2[:, 128:]

    acc[...] = jnp.zeros_like(acc)

    @pl.loop(0, 23)
    def _(s):
        @pl.when(jnp.logical_and(s < 16, inner))
        def _():
            here = place(source(s, 0))
            copy(relay.at[here], relay.at[here], l_send.at[0], l_recv.at[here], mirror).wait_recv()
            relayed(s).start()

        a = s - LAG1

        @pl.when(jnp.logical_and(a >= 0, a < 16))
        def _():
            slot = xl * 32 + source(a, 0)
            arrived(slot)
            forward(slot, a, nbr)
            forward(slot, 16 + a, peer)

        b = s - LAG1 - LAG2

        @pl.when(jnp.logical_and(b >= 0, b < 16))
        def _():
            slot = (1 - xl) * 32 + source(b, 0)
            arrived(slot)
            forward(slot, 32 + b, peer)

        @pl.when(s == 3)
        def _():
            pltpu.make_async_copy(rsend, rm, r_recv).wait()

            @pl.when(second)
            def _():
                r_copy(rm, 0).start()

        @pl.when(s == 6)
        def _():
            build_lhs()

        @pl.when(s >= FIRST)
        def _():
            @pl.loop(0, jnp.where(jnp.logical_or(s == FIRST + 9, s == FIRST + 11), 2, 1))
            def _(v):
                w = jnp.where(s == FIRST + 9, 7, 11)
                for k, first in enumerate(UNITS):
                    w = jnp.where(jnp.logical_and(v == 0, s == FIRST + k), first, w)
                unit(w)

    mags = nt(eye, rm[TILES * 16 :, :])
    for j in range(TILES):
        squares = jnp.sum(acc[j * 128 : (j + 1) * 128, :], axis=1, keepdims=True)
        scale = jnp.broadcast_to(mags[:, j : j + 1] / jnp.sqrt(squares + 1e-6), (128, 128))
        for g in range(4):
            scale_ref[pl.ds(starts[j][g], 32), :] = scale[32 * g : 32 * g + 32]

    for k in range(16):

        @pl.when(outgoing(k)[2])
        def _():
            copy(send_buf.at[0], relay.at[0], a_send.at[k], l_recv.at[0], mirror).wait_send()

    @pl.loop(0, 16)
    def _(k):
        @pl.when(inner)
        def _():
            relayed(k).wait_send()

    @pl.loop(0, 48)
    def _(k):
        copy(recv.at[0], recv.at[0], f_send.at[k], recv_sem.at[0], (t, peer)).wait_send()

    @pl.when(mine)
    def _():
        for k in range(2):
            r_copy(rsend, k).wait_send()

    @pl.when(second)
    def _():
        r_copy(rm, 0).wait_send()


def scale_kernel(merged, scale, out_hbm, out_ref, sems):
    def written(k):
        rows = pl.ds(k * 128, 128)
        return pltpu.make_async_copy(out_ref.at[rows], out_hbm.at[rows], sems.at[k])

    for k in range(TILES):

        @pl.loop(0, 8)
        def _(n):
            rows = pl.ds(pl.multiple_of(k * 128 + n * 16, 16), 16)
            s = scale[rows, :]
            for i in range(T * ROWS // 128):
                cols = slice(i * 128, i * 128 + 128)
                out_ref[rows, cols] = (merged[rows, cols] * s).astype(BF16)

        written(k).start()
    for k in range(TILES):
        written(k).wait()


def shards(base_weight, adapter_left, adapter_right, magnitude):
    x = base_weight.reshape(EPS, ROWS, 3584)
    left = jnp.swapaxes(adapter_left, 2, 3).reshape(EPS, 16, ROWS)
    right = adapter_right.reshape(EPS, 16, 3584)
    x, left, right, magnitude = (pltpu.with_memory_space_constraint(a, pltpu.HBM) for a in (x, left, right, magnitude))
    vmem = pl.BlockSpec(memory_space=pltpu.VMEM)
    merged, scale = pl.pallas_call(
        exchange_kernel,
        out_shape=(pltpu.VMEM((EPS * SERVE, T * ROWS), F32), pltpu.VMEM((EPS * SERVE, 128), F32)),
        in_specs=[pl.BlockSpec(memory_space=pltpu.HBM)] * 4,
        out_specs=(vmem, vmem),
        scratch_shapes=[
            pltpu.VMEM((EPS, ROWS, 3584), BF16),
            pltpu.VMEM((EPS, 16, ROWS), BF16),
            pltpu.VMEM((EPS, 16, 3584), BF16),
            pltpu.VMEM((2, 2, 3584), BF16),
            pltpu.SemaphoreType.DMA((7,)),
            pltpu.VMEM((16, BROWS, 128), BF16),
            pltpu.VMEM((RROWS, 128), BF16),
            pltpu.VMEM((T, BROWS, 128), BF16),
            pltpu.VMEM((16, BROWS, 128), BF16),
            pltpu.VMEM((RROWS, 128), BF16),
            pltpu.VMEM((EPS * SERVE, 128), F32),
            pltpu.VMEM((TILES, 128, 256), BF16),
            pltpu.SemaphoreType.DMA((16,)),
            pltpu.SemaphoreType.DMA((16,)),
            pltpu.SemaphoreType.DMA((48,)),
            pltpu.SemaphoreType.DMA((2,)),
            pltpu.SemaphoreType.DMA((T,)),
            pltpu.SemaphoreType.DMA((16,)),
            pltpu.SemaphoreType.DMA,
        ],
        compiler_params=pltpu.CompilerParams(collective_id=0, has_side_effects=True, vmem_limit_bytes=24 * 2**20),
        name="exchange",
    )(x, left, right, magnitude)
    out = pl.pallas_call(
        scale_kernel,
        out_shape=jax.ShapeDtypeStruct((EPS * SERVE, T * ROWS), BF16),
        in_specs=[vmem, vmem],
        out_specs=pl.BlockSpec(memory_space=pltpu.HBM),
        scratch_shapes=[pltpu.VMEM((EPS * SERVE, T * ROWS), BF16), pltpu.SemaphoreType.DMA((TILES,))],
        compiler_params=pltpu.CompilerParams(vmem_limit_bytes=16 * 2**20),
        name="scale",
    )(merged, scale)
    return out.reshape(2, 2, SERVE, T * ROWS)


def solution(mesh):
    in_specs = (
        P(None, None, "tensor", "dp"),
        P(None, None, "tensor", None),
        P(None, None, None, "dp"),
        P(None, None, "dp"),
    )
    out_specs = P(None, None, "tensor", None)
    return jax.shard_map(shards, mesh=mesh, in_specs=in_specs, out_specs=out_specs, check_vma=False)
```

```python
import functools

import jax
import jax.numpy as jnp
from jax import lax
from jax.experimental import pallas as pl
from jax.experimental.pallas import tpu as pltpu
from jax.sharding import PartitionSpec as P

MESH = pl.DeviceIdType.MESH
F32, BF16 = jnp.float32, jnp.bfloat16

T = 64
ROWS = 64
SERVE = 224
EPS = 4
TILES = 7
WROWS = TILES * ROWS
LROWS = 32
RROWS = TILES * 16 + 16
LAG1, LAG2 = 2, 2
FIRST = 9
UNITS = ((0,), (1,), (4,), (2,), (5,), (3,), (8,), (6,), (9, 7), (12, 10, 11), (13, 14), (15,))


def packed(load, m):
    hole = 3 - m
    full = [load(e, 2 * m) for e in range(EPS)]
    rest = []
    for e in range(EPS):
        if m == 0:
            rest.append(load(e, 1))
        elif m == 3:
            rest.append(load(e, 5))
        else:
            low, high = load(e, 2 * m + 1), load(e, 2 * m - 1)
            group = lax.broadcasted_iota(jnp.int32, low.shape, 1) // 32
            rest.append(jnp.where(group < hole, low, high))
    last = rest[3].astype(F32)
    group = lax.broadcasted_iota(jnp.int32, last.shape, 1) // 32
    for k in range(3):
        full.append(jnp.where(group == hole, pltpu.roll(last, 32 * (k + 1), 1).astype(BF16), rest[k]))
    return full


def nt(a, b):
    return lax.dot_general(a, b, (((1,), (1,)), ((), ())), preferred_element_type=F32)


SENDS = tuple((d, p) for d in (0, 1, -1, 2, -2, 3, -3, 4) for p in (0, 1))


def arrival(s):
    even = lax.rem(s, 2) == 0
    far = jnp.where(s >= 10, 3, 2)
    dz_near = jnp.where(jnp.logical_or(s == 0, s == 5), 0, jnp.where(even, -1, 1))
    dz_far = jnp.where(s >= 14, 4, jnp.where(even, far, -far))
    late = jnp.where(s < 6, s >= 3, jnp.where(s < 10, s >= 8, jnp.where(s < 14, s >= 12, s == 15)))
    return jnp.where(s < 6, dz_near, dz_far), late


def exchange_kernel(
    x_hbm, l_hbm, r_hbm, m_hbm, merged, scale_ref, x_ref, l_ref, r_ref, m_ref, in_sem, send_buf, rsend, recv, relay, rm, acc, lhs, lall, a_send, l_send, f_send, r_send, recv_sem, l_recv, r_recv, g_send, g_recv
):
    t, q = lax.axis_index("tensor"), lax.axis_index("dp")
    xh, y, z = t // 32, (t // 8) % 4, t % 8
    xl, c = q // 2, q % 2
    nbr, peer = q + 2 - 4 * xl, q + 1 - 2 * c
    edge, inner = xh == xl, xh != xl
    mirror = (xl * 32 + y * 8 + z, 2 * xh + c)
    src_core, dst_core = y // 2, y % 2
    row_m = t % 4
    hole = 3 - row_m

    y_rows = [[(y + (y + parity) % 2 + 2 * w) % 4 * 8 for w in range(2)] for parity in (c, 1 - c)]

    def source(s, who):
        dz, late = arrival(s)
        return jnp.where(late, y_rows[who][1], y_rows[who][0]) + lax.rem(z - dz + 8, 8)

    def place(yz):
        return lax.div(yz, 16) * 8 + lax.rem(yz, 8)

    small_in = [pltpu.make_async_copy(a, b, in_sem.at[4 + k]) for k, (a, b) in enumerate(((l_hbm, l_ref), (r_hbm, r_ref), (m_hbm, m_ref)))]

    def x_in(g):
        cols = pl.ds(pl.multiple_of(g * (TILES * 128), 128), TILES * 128)
        return pltpu.make_async_copy(x_hbm.at[:, :, cols], x_ref.at[:, :, cols], in_sem.at[g])

    for a in small_in:
        a.start()
    for g in range(4):
        x_in(g).start()

    barrier = pltpu.get_barrier_semaphore()

    @pl.loop(0, 16)
    def _(s):
        yz = source(s, 0)

        @pl.when(jnp.logical_or(yz != y * 8 + z, src_core != c))
        def _():
            pl.semaphore_signal(barrier, inc=1, device_id=(xh * 32 + yz, xl * 2 + src_core), device_id_type=MESH)

    opposite = ((1 - xh) * 32 + y * 8 + z, (1 - xl) * 2 + c)

    def z_partner(k):
        return (xh * 32 + y * 8 + (z + k) % 8, q)

    def y_partner(k):
        return (xh * 32 + (y + k) % 4 * 8 + z, q)

    greeted = [(t, nbr), (t, peer), opposite] + [z_partner(k) for k in range(1, 8)] + [y_partner(k) for k in range(1, 4)]
    for other in greeted:
        pl.semaphore_signal(barrier, inc=1, device_id=other, device_id_type=MESH)

    for a in small_in:
        a.wait()
    lanes = lax.broadcasted_iota(jnp.int32, (16, 128), 1)
    ranks = lax.broadcasted_iota(jnp.int32, (16, 128), 0)
    lpack = jnp.zeros((LROWS, 128), F32)
    for e in range(EPS):
        low = (lanes == e * 16 + ranks).astype(BF16)
        high = (lanes == 64 + e * 16 + ranks).astype(BF16)
        tn = functools.partial(lax.dot_general, dimension_numbers=(((0,), (0,)), ((), ())), preferred_element_type=F32)
        lpack += tn(l_ref[e], low)[:LROWS] + tn(l_ref[e], high)[LROWS:]
    lall[c, y, z, xh] = jnp.where(c == 0, lpack[:16], lpack[16:]).astype(BF16)

    @pl.loop(0, 4)
    def _(g):
        base = g * (TILES * 128)
        x_in(g).wait()

        def at(k):
            return pl.ds(pl.multiple_of(base + 128 * k, 128), 128)

        for m in range(4):
            d = g * 4 + m
            for j, tile in enumerate(packed(lambda e, k: x_ref[e, :, at(k)], m)):
                send_buf[d, j * ROWS : (j + 1) * ROWS, :] = tile

    mine = q == t // 16
    for m in range(4):

        @pl.when(jnp.logical_and(mine, row_m == m))
        def _():
            base = t % 16 // 4 * (TILES * 128)

            def at(k):
                return pl.ds(pl.multiple_of(base + 128 * k, 128), 128)

            rt = packed(lambda e, k: r_ref[e, :, at(k)], m)
            mt = packed(lambda e, k: jnp.broadcast_to(m_ref[e // 2, :, at(k)].astype(F32)[e % 2 : e % 2 + 1], (16, 128)).astype(BF16), m)
            mags = jnp.zeros((16, 128), F32)
            for j in range(TILES):
                rsend[j * 16 : j * 16 + 16, :] = rt[j]
                mags = jnp.where(ranks == j, mt[j].astype(F32), mags)
            rsend[TILES * 16 :, :] = mags.astype(BF16)

    self_out = jnp.logical_and(src_core == c, dst_core == c).astype(jnp.int32)
    pl.semaphore_wait(barrier, 16 + len(greeted) - self_out)

    def copy(src, dst, send, recv_s, dev):
        return pltpu.make_async_remote_copy(
            src_ref=src, dst_ref=dst, send_sem=send, recv_sem=recv_s, device_id=dev, device_id_type=MESH
        )

    second = nbr == t // 16

    def r_copy(src, k):
        return copy(src, rm, r_send.at[k], r_recv, (t, (peer, nbr)[k]))

    @pl.when(mine)
    def _():
        for k in range(2):
            r_copy(rsend, k).start()
        pltpu.make_async_copy(rsend, rm, r_recv).start()

    def outgoing(k):
        dz, p = SENDS[k]
        yd, zd = 2 * c + (y + p) % 2, (z + dz + 8) % 8
        away = jnp.logical_or(jnp.logical_or(yd != y, zd != z), dst_core != c)
        return yd, zd, away

    own = place(y * 8 + z)

    def send(k):
        yd, zd, away = outgoing(k)
        dev = (xh * 32 + yd * 8 + zd, xl * 2 + dst_core)
        block = send_buf.at[(yd - 2 * c) * 8 + zd]

        @pl.when(jnp.logical_and(away, edge))
        def _():
            copy(block, recv.at[t], a_send.at[k], recv_sem.at[t], dev).start()

        @pl.when(jnp.logical_and(away, inner))
        def _():
            copy(block, relay.at[own], a_send.at[k], l_recv.at[own], dev).start()

        @pl.when(jnp.logical_and(jnp.logical_not(away), edge))
        def _():
            pltpu.make_async_copy(block, recv.at[t], recv_sem.at[t]).start()

        @pl.when(jnp.logical_and(jnp.logical_not(away), inner))
        def _():
            pltpu.make_async_copy(block, relay.at[own], l_recv.at[own]).start()

    def left_copy(ref, k, dev):
        return copy(ref, ref, g_send.at[k], g_recv.at[k], dev)

    left_x = left_copy(lall.at[c, y, z, xh], 0, opposite)
    left_z = [left_copy(lall.at[c, y, z], k, z_partner(k)) for k in range(1, 8)]
    left_y = [left_copy(lall.at[c, y], 7 + k, y_partner(k)) for k in range(1, 4)]
    left_core = left_copy(lall.at[c], 11, (t, peer))

    left_x.start()
    for k in range(6):
        send(k)
    left_copy(lall.at[c, y, z, 1 - xh], 0, opposite).wait_recv()
    for m in left_z:
        m.start()
    for k in range(6, 10):
        send(k)

    def arrived(slot):
        copy(recv.at[slot], recv.at[slot], f_send.at[0], recv_sem.at[slot], (t, peer)).wait_recv()

    def forward(slot, k, other):
        copy(recv.at[slot], recv.at[slot], f_send.at[k], recv_sem.at[slot], (t, other)).start()

    def relayed(s):
        yz = source(s, 0)
        slot = xh * 32 + yz
        return copy(relay.at[place(yz)], recv.at[slot], l_send.at[s], recv_sem.at[slot], mirror)

    lane = lax.broadcasted_iota(jnp.int32, (128, 128), 1)
    row = lax.broadcasted_iota(jnp.int32, (128, 128), 0)
    eye = (lane == row).astype(BF16)

    def build_lhs():
        for j in range(TILES):
            r = rm[j * 16 : j * 16 + 16, :].astype(F32)
            r8 = jnp.concatenate([r] * 8, axis=0)
            e_lane = j if j < 4 else jnp.where(lane // 32 == hole, 3, j - 4)
            rbd = jnp.where((row // 16) % 4 == e_lane, r8, 0.0).astype(BF16)
            lhs[j, :, 0:128] = eye
            lhs[j, :, 128:256] = nt(eye, rbd).astype(BF16)

    def column(g):
        return jnp.where(g > hole, 32 * (g - hole - 1), 128 + 32 * row_m + 32 * g)

    def row_start(j, g):
        if j < 4:
            return pl.multiple_of(SERVE * j + 32 * row_m + 32 * g, 32)
        k = j - 4
        from3 = (hole - k - 1 + 4) % 4
        return pl.multiple_of(jnp.where(hole == g, SERVE * 3 + column(from3), SERVE * k + column(g)), 32)

    starts = [[row_start(j, g) for g in range(4)] for j in range(TILES)]
    low_half = lax.broadcasted_iota(jnp.int32, (LROWS, 128), 1) < 64

    def unit(w):
        stage, who = w // 4, w % 4
        half = jnp.where(who % 2 == 1, 1 - xl, xl)
        parity = jnp.where(who >= 2, 1 - c, c)
        odd = z % 2
        step = jnp.where(stage == 0, 0, jnp.where(stage == 1, -2, jnp.where(stage == 2, 2, 4)))
        zp = (z - odd + (1 - 2 * odd) * step + 8) % 8
        firsts = [half * 32 + (parity + 2 * h) * 8 + zp for h in range(2)]
        slots = [f + k for f in firsts for k in range(2)]

        @pl.when(who >= 2)
        def _():
            @pl.loop(jnp.where(stage == 0, 0, 2 + 4 * stage), jnp.where(stage == 3, 16, 6 + 4 * stage))
            def _(i):
                arrived(half * 32 + source(i, 1))

        parts = []
        for h, k in ((0, 0), (0, 1), (1, 0), (1, 1)):
            lb = jnp.concatenate([lall[n, parity + 2 * h, zp + k, half] for n in range(2)], axis=0).astype(F32)
            parts += [jnp.where(low_half, lb, 0.0), jnp.where(low_half, 0.0, lb)]
        lm = jnp.concatenate(parts, axis=0).astype(BF16)
        for j in range(TILES):
            wt = jnp.concatenate([recv[s, j * ROWS : (j + 1) * ROWS, :] for s in slots], axis=0)
            o = nt(lhs[j], jnp.concatenate([wt, lm], axis=1))
            for h in range(2):
                cols = pl.ds(pl.multiple_of(firsts[h] * 64, 128), 128)
                if j < 4:
                    merged[pl.ds(starts[j][0], 128), cols] = o[:, 128 * h : 128 * h + 128]
                else:
                    for g in range(4):
                        merged[pl.ds(starts[j][g], 32), cols] = o[32 * g : 32 * g + 32, 128 * h : 128 * h + 128]
            o2 = o * o
            acc[j * 128 : (j + 1) * 128, :] += o2[:, :128] + o2[:, 128:]

    acc[...] = jnp.zeros_like(acc)

    @pl.loop(0, FIRST + len(UNITS))
    def _(s):
        @pl.when(jnp.logical_and(s < 16, inner))
        def _():
            here = place(source(s, 0))
            copy(relay.at[here], relay.at[here], l_send.at[0], l_recv.at[here], mirror).wait_recv()
            relayed(s).start()

        a = s - LAG1

        @pl.when(jnp.logical_and(a >= 0, a < 16))
        def _():
            slot = xl * 32 + source(a, 0)
            arrived(slot)
            forward(slot, a, nbr)
            forward(slot, 16 + a, peer)

        b = s - LAG1 - LAG2

        @pl.when(jnp.logical_and(b >= 0, b < 16))
        def _():
            slot = (1 - xl) * 32 + source(b, 0)
            arrived(slot)
            forward(slot, 32 + b, peer)

        @pl.when(s == 2)
        def _():
            for k in range(1, 8):
                left_copy(lall.at[c, y, (z - k + 8) % 8], k, z_partner(k)).wait_recv()
            for m in left_y:
                m.start()
            for k in range(10, 16):
                send(k)

        @pl.when(s == 7)
        def _():
            for k in range(1, 4):
                left_copy(lall.at[c, (y - k + 4) % 4], 7 + k, y_partner(k)).wait_recv()
            left_core.start()

        @pl.when(s == 8)
        def _():
            left_copy(lall.at[1 - c], 11, (t, peer)).wait_recv()

        @pl.when(s == 3)
        def _():
            pltpu.make_async_copy(rsend, rm, r_recv).wait()

            @pl.when(second)
            def _():
                r_copy(rm, 0).start()

        @pl.when(s == 6)
        def _():
            build_lhs()

        @pl.when(s >= FIRST)
        def _():
            count = 1
            for k, some in enumerate(UNITS):
                count = jnp.where(s == FIRST + k, len(some), count)

            @pl.loop(0, count)
            def _(v):
                w = 0
                for k, some in enumerate(UNITS):
                    for n, u in enumerate(some):
                        w = jnp.where(jnp.logical_and(v == n, s == FIRST + k), u, w)
                unit(w)

    mags = nt(eye, rm[TILES * 16 :, :])
    for j in range(TILES):
        squares = jnp.sum(acc[j * 128 : (j + 1) * 128, :], axis=1, keepdims=True)
        scale = jnp.broadcast_to(mags[:, j : j + 1] / jnp.sqrt(squares + 1e-6), (128, 128))
        for g in range(4):
            scale_ref[pl.ds(starts[j][g], 32), :] = scale[32 * g : 32 * g + 32]

    for m in [left_x, left_core] + left_z + left_y:
        m.wait_send()
    for k in range(16):

        @pl.when(outgoing(k)[2])
        def _():
            copy(send_buf.at[0], relay.at[0], a_send.at[k], l_recv.at[0], mirror).wait_send()

    @pl.loop(0, 16)
    def _(k):
        @pl.when(inner)
        def _():
            relayed(k).wait_send()

    @pl.loop(0, 48)
    def _(k):
        copy(recv.at[0], recv.at[0], f_send.at[k], recv_sem.at[0], (t, peer)).wait_send()

    @pl.when(mine)
    def _():
        for k in range(2):
            r_copy(rsend, k).wait_send()

    @pl.when(second)
    def _():
        r_copy(rm, 0).wait_send()


def scale_kernel(merged, scale, out_hbm, out_ref, sems):
    def written(k):
        rows = pl.ds(k * 128, 128)
        return pltpu.make_async_copy(out_ref.at[rows], out_hbm.at[rows], sems.at[k])

    for k in range(TILES):

        @pl.loop(0, 8)
        def _(n):
            rows = pl.ds(pl.multiple_of(k * 128 + n * 16, 16), 16)
            s = scale[rows, :]
            for i in range(T * ROWS // 128):
                cols = slice(i * 128, i * 128 + 128)
                out_ref[rows, cols] = (merged[rows, cols] * s).astype(BF16)

        written(k).start()
    for k in range(TILES):
        written(k).wait()


def shards(base_weight, adapter_left, adapter_right, magnitude):
    x = base_weight.reshape(EPS, ROWS, 3584)
    left = jnp.swapaxes(adapter_left, 2, 3).reshape(EPS, 16, ROWS)
    right = adapter_right.reshape(EPS, 16, 3584)
    x, left, right, magnitude = (pltpu.with_memory_space_constraint(a, pltpu.HBM) for a in (x, left, right, magnitude))
    vmem = pl.BlockSpec(memory_space=pltpu.VMEM)
    merged, scale = pl.pallas_call(
        exchange_kernel,
        out_shape=(pltpu.VMEM((EPS * SERVE, T * ROWS), F32), pltpu.VMEM((EPS * SERVE, 128), F32)),
        in_specs=[pl.BlockSpec(memory_space=pltpu.HBM)] * 4,
        out_specs=(vmem, vmem),
        scratch_shapes=[
            pltpu.VMEM((EPS, ROWS, 3584), BF16),
            pltpu.VMEM((EPS, 16, ROWS), BF16),
            pltpu.VMEM((EPS, 16, 3584), BF16),
            pltpu.VMEM((2, 2, 3584), BF16),
            pltpu.SemaphoreType.DMA((7,)),
            pltpu.VMEM((16, WROWS, 128), BF16),
            pltpu.VMEM((RROWS, 128), BF16),
            pltpu.VMEM((T, WROWS, 128), BF16),
            pltpu.VMEM((16, WROWS, 128), BF16),
            pltpu.VMEM((RROWS, 128), BF16),
            pltpu.VMEM((EPS * SERVE, 128), F32),
            pltpu.VMEM((TILES, 128, 256), BF16),
            pltpu.VMEM((2, 4, 8, 2, LROWS // 2, 128), BF16),
            pltpu.SemaphoreType.DMA((16,)),
            pltpu.SemaphoreType.DMA((16,)),
            pltpu.SemaphoreType.DMA((48,)),
            pltpu.SemaphoreType.DMA((2,)),
            pltpu.SemaphoreType.DMA((T,)),
            pltpu.SemaphoreType.DMA((16,)),
            pltpu.SemaphoreType.DMA,
            pltpu.SemaphoreType.DMA((12,)),
            pltpu.SemaphoreType.DMA((12,)),
        ],
        compiler_params=pltpu.CompilerParams(collective_id=0, has_side_effects=True, vmem_limit_bytes=24 * 2**20),
        name="exchange",
    )(x, left, right, magnitude)
    out = pl.pallas_call(
        scale_kernel,
        out_shape=jax.ShapeDtypeStruct((EPS * SERVE, T * ROWS), BF16),
        in_specs=[vmem, vmem],
        out_specs=pl.BlockSpec(memory_space=pltpu.HBM),
        scratch_shapes=[pltpu.VMEM((EPS * SERVE, T * ROWS), BF16), pltpu.SemaphoreType.DMA((TILES,))],
        compiler_params=pltpu.CompilerParams(vmem_limit_bytes=16 * 2**20),
        name="scale",
    )(merged, scale)
    return out.reshape(2, 2, SERVE, T * ROWS)


def solution(mesh):
    in_specs = (
        P(None, None, "tensor", "dp"),
        P(None, None, "tensor", None),
        P(None, None, None, "dp"),
        P(None, None, "dp"),
    )
    out_specs = P(None, None, "tensor", None)
    return jax.shard_map(shards, mesh=mesh, in_specs=in_specs, out_specs=out_specs, check_vma=False)
```

```python
import functools

import jax
import jax.numpy as jnp
from jax import lax
from jax.experimental import pallas as pl
from jax.experimental.pallas import tpu as pltpu
from jax.sharding import PartitionSpec as P

MESH = pl.DeviceIdType.MESH
F32, BF16 = jnp.float32, jnp.bfloat16

T = 64
ROWS = 64
SERVE = 224
EPS = 4
TILES = 7
WROWS = TILES * ROWS
LROWS = 32
RROWS = TILES * 16 + 16
LAG1, LAG2 = 2, 2
FIRST = 9
UNITS = ((0,), (1,), (4,), (2,), (5,), (3,), (8,), (6,), (9, 7), (12, 10, 11), (13, 14), (15,))


def packed(load, m):
    hole = 3 - m
    full = [load(e, 2 * m) for e in range(EPS)]
    rest = []
    for e in range(EPS):
        if m == 0:
            rest.append(load(e, 1))
        elif m == 3:
            rest.append(load(e, 5))
        else:
            low, high = load(e, 2 * m + 1), load(e, 2 * m - 1)
            group = lax.broadcasted_iota(jnp.int32, low.shape, 1) // 32
            rest.append(jnp.where(group < hole, low, high))
    last = rest[3].astype(F32)
    group = lax.broadcasted_iota(jnp.int32, last.shape, 1) // 32
    for k in range(3):
        full.append(jnp.where(group == hole, pltpu.roll(last, 32 * (k + 1), 1).astype(BF16), rest[k]))
    return full


def nt(a, b):
    return lax.dot_general(a, b, (((1,), (1,)), ((), ())), preferred_element_type=F32)


SENDS = tuple((d, p) for d in (0, 1, -1, 2, -2, 3, -3, 4) for p in (0, 1))


def arrival(s):
    even = lax.rem(s, 2) == 0
    far = jnp.where(s >= 10, 3, 2)
    dz_near = jnp.where(jnp.logical_or(s == 0, s == 5), 0, jnp.where(even, -1, 1))
    dz_far = jnp.where(s >= 14, 4, jnp.where(even, far, -far))
    late = jnp.where(s < 6, s >= 3, jnp.where(s < 10, s >= 8, jnp.where(s < 14, s >= 12, s == 15)))
    return jnp.where(s < 6, dz_near, dz_far), late


def exchange_kernel(
    x_hbm, l_hbm, r_hbm, m_hbm, merged, scale_ref, x_ref, l_ref, r_ref, m_ref, in_sem, send_buf, rsend, recv, relay, rm, acc, lhs, lall, a_send, l_send, f_send, r_send, recv_sem, l_recv, r_recv, g_send, g_recv
):
    t, q = lax.axis_index("tensor"), lax.axis_index("dp")
    xh, y, z = t // 32, (t // 8) % 4, t % 8
    xl, c = q // 2, q % 2
    nbr, peer = q + 2 - 4 * xl, q + 1 - 2 * c
    edge, inner = xh == xl, xh != xl
    mirror = (xl * 32 + y * 8 + z, 2 * xh + c)
    src_core, dst_core = y // 2, y % 2
    row_m = t % 4
    hole = 3 - row_m

    y_rows = [[(y + (y + parity) % 2 + 2 * w) % 4 * 8 for w in range(2)] for parity in (c, 1 - c)]

    def source(s, who):
        dz, late = arrival(s)
        return jnp.where(late, y_rows[who][1], y_rows[who][0]) + lax.rem(z - dz + 8, 8)

    def place(yz):
        return lax.div(yz, 16) * 8 + lax.rem(yz, 8)

    small_in = [pltpu.make_async_copy(a, b, in_sem.at[4 + k]) for k, (a, b) in enumerate(((l_hbm, l_ref), (r_hbm, r_ref), (m_hbm, m_ref)))]

    def x_in(g):
        cols = pl.ds(pl.multiple_of(g * (TILES * 128), 128), TILES * 128)
        return pltpu.make_async_copy(x_hbm.at[:, :, cols], x_ref.at[:, :, cols], in_sem.at[g])


    barrier = pltpu.get_barrier_semaphore()

    for n in range(16):
        yz = source(15 - n, 0)

        @pl.when(jnp.logical_or(yz != y * 8 + z, src_core != c))
        def _():
            pl.semaphore_signal(barrier, inc=1, device_id=(xh * 32 + yz, xl * 2 + src_core), device_id_type=MESH)

    opposite = ((1 - xh) * 32 + y * 8 + z, (1 - xl) * 2 + c)

    def z_partner(k):
        return (xh * 32 + y * 8 + (z + k) % 8, q)

    def y_partner(k):
        return (xh * 32 + (y + k) % 4 * 8 + z, q)

    greeted = [z_partner(k) for k in (4, 3, 5, 2, 6, 1, 7)] + [(t, nbr), (t, peer), opposite] + [y_partner(k) for k in range(1, 4)]
    for other in greeted:
        pl.semaphore_signal(barrier, inc=1, device_id=other, device_id_type=MESH)

    for a in small_in:
        a.start()
    for g in range(4):
        x_in(g).start()

    for a in small_in:
        a.wait()
    lanes = lax.broadcasted_iota(jnp.int32, (16, 128), 1)
    ranks = lax.broadcasted_iota(jnp.int32, (16, 128), 0)
    lpack = jnp.zeros((LROWS, 128), F32)
    for e in range(EPS):
        low = (lanes == e * 16 + ranks).astype(BF16)
        high = (lanes == 64 + e * 16 + ranks).astype(BF16)
        tn = functools.partial(lax.dot_general, dimension_numbers=(((0,), (0,)), ((), ())), preferred_element_type=F32)
        lpack += tn(l_ref[e], low)[:LROWS] + tn(l_ref[e], high)[LROWS:]
    lall[c, y, z, xh] = jnp.where(c == 0, lpack[:16], lpack[16:]).astype(BF16)

    @pl.loop(0, 4)
    def _(g):
        base = g * (TILES * 128)
        x_in(g).wait()

        def at(k):
            return pl.ds(pl.multiple_of(base + 128 * k, 128), 128)

        for m in range(4):
            d = g * 4 + m
            for j, tile in enumerate(packed(lambda e, k: x_ref[e, :, at(k)], m)):
                send_buf[d, j * ROWS : (j + 1) * ROWS, :] = tile

    mine = q == t // 16
    for m in range(4):

        @pl.when(jnp.logical_and(mine, row_m == m))
        def _():
            base = t % 16 // 4 * (TILES * 128)

            def at(k):
                return pl.ds(pl.multiple_of(base + 128 * k, 128), 128)

            rt = packed(lambda e, k: r_ref[e, :, at(k)], m)
            mt = packed(lambda e, k: jnp.broadcast_to(m_ref[e // 2, :, at(k)].astype(F32)[e % 2 : e % 2 + 1], (16, 128)).astype(BF16), m)
            mags = jnp.zeros((16, 128), F32)
            for j in range(TILES):
                rsend[j * 16 : j * 16 + 16, :] = rt[j]
                mags = jnp.where(ranks == j, mt[j].astype(F32), mags)
            rsend[TILES * 16 :, :] = mags.astype(BF16)

    self_out = jnp.logical_and(src_core == c, dst_core == c).astype(jnp.int32)
    pl.semaphore_wait(barrier, 16 + len(greeted) - self_out)

    def copy(src, dst, send, recv_s, dev):
        return pltpu.make_async_remote_copy(
            src_ref=src, dst_ref=dst, send_sem=send, recv_sem=recv_s, device_id=dev, device_id_type=MESH
        )

    second = nbr == t // 16

    def r_copy(src, k):
        return copy(src, rm, r_send.at[k], r_recv, (t, (peer, nbr)[k]))

    @pl.when(mine)
    def _():
        for k in range(2):
            r_copy(rsend, k).start()
        pltpu.make_async_copy(rsend, rm, r_recv).start()

    def outgoing(k):
        dz, p = SENDS[k]
        yd, zd = 2 * c + (y + p) % 2, (z + dz + 8) % 8
        away = jnp.logical_or(jnp.logical_or(yd != y, zd != z), dst_core != c)
        return yd, zd, away

    own = place(y * 8 + z)

    def send(k):
        yd, zd, away = outgoing(k)
        dev = (xh * 32 + yd * 8 + zd, xl * 2 + dst_core)
        block = send_buf.at[(yd - 2 * c) * 8 + zd]

        @pl.when(jnp.logical_and(away, edge))
        def _():
            copy(block, recv.at[t], a_send.at[k], recv_sem.at[t], dev).start()

        @pl.when(jnp.logical_and(away, inner))
        def _():
            copy(block, relay.at[own], a_send.at[k], l_recv.at[own], dev).start()

        @pl.when(jnp.logical_and(jnp.logical_not(away), edge))
        def _():
            pltpu.make_async_copy(block, recv.at[t], recv_sem.at[t]).start()

        @pl.when(jnp.logical_and(jnp.logical_not(away), inner))
        def _():
            pltpu.make_async_copy(block, relay.at[own], l_recv.at[own]).start()

    def left_copy(ref, k, dev):
        return copy(ref, ref, g_send.at[k], g_recv.at[k], dev)

    left_x = left_copy(lall.at[c, y, z, xh], 0, opposite)
    left_z = [left_copy(lall.at[c, y, z], k, z_partner(k)) for k in range(1, 8)]
    left_y = [left_copy(lall.at[c, y], 7 + k, y_partner(k)) for k in range(1, 4)]
    left_core = left_copy(lall.at[c], 11, (t, peer))

    left_x.start()
    for k in range(6):
        send(k)
    left_copy(lall.at[c, y, z, 1 - xh], 0, opposite).wait_recv()
    for m in left_z:
        m.start()
    for k in range(6, 10):
        send(k)

    def arrived(slot):
        copy(recv.at[slot], recv.at[slot], f_send.at[0], recv_sem.at[slot], (t, peer)).wait_recv()

    def forward(slot, k, other):
        copy(recv.at[slot], recv.at[slot], f_send.at[k], recv_sem.at[slot], (t, other)).start()

    def relayed(s):
        yz = source(s, 0)
        slot = xh * 32 + yz
        return copy(relay.at[place(yz)], recv.at[slot], l_send.at[s], recv_sem.at[slot], mirror)

    lane = lax.broadcasted_iota(jnp.int32, (128, 128), 1)
    row = lax.broadcasted_iota(jnp.int32, (128, 128), 0)
    eye = (lane == row).astype(BF16)

    def build_lhs():
        for j in range(TILES):
            r = rm[j * 16 : j * 16 + 16, :].astype(F32)
            r8 = jnp.concatenate([r] * 8, axis=0)
            e_lane = j if j < 4 else jnp.where(lane // 32 == hole, 3, j - 4)
            rbd = jnp.where((row // 16) % 4 == e_lane, r8, 0.0).astype(BF16)
            lhs[j, :, 0:128] = eye
            lhs[j, :, 128:256] = nt(eye, rbd).astype(BF16)

    def column(g):
        return jnp.where(g > hole, 32 * (g - hole - 1), 128 + 32 * row_m + 32 * g)

    def row_start(j, g):
        if j < 4:
            return pl.multiple_of(SERVE * j + 32 * row_m + 32 * g, 32)
        k = j - 4
        from3 = (hole - k - 1 + 4) % 4
        return pl.multiple_of(jnp.where(hole == g, SERVE * 3 + column(from3), SERVE * k + column(g)), 32)

    starts = [[row_start(j, g) for g in range(4)] for j in range(TILES)]
    low_half = lax.broadcasted_iota(jnp.int32, (LROWS, 128), 1) < 64

    def unit(w):
        stage, who = w // 4, w % 4
        half = jnp.where(who % 2 == 1, 1 - xl, xl)
        parity = jnp.where(who >= 2, 1 - c, c)
        odd = z % 2
        step = jnp.where(stage == 0, 0, jnp.where(stage == 1, -2, jnp.where(stage == 2, 2, 4)))
        zp = (z - odd + (1 - 2 * odd) * step + 8) % 8
        firsts = [half * 32 + (parity + 2 * h) * 8 + zp for h in range(2)]
        slots = [f + k for f in firsts for k in range(2)]

        @pl.when(who >= 2)
        def _():
            @pl.loop(jnp.where(stage == 0, 0, 2 + 4 * stage), jnp.where(stage == 3, 16, 6 + 4 * stage))
            def _(i):
                arrived(half * 32 + source(i, 1))

        parts = []
        for h, k in ((0, 0), (0, 1), (1, 0), (1, 1)):
            lb = jnp.concatenate([lall[n, parity + 2 * h, zp + k, half] for n in range(2)], axis=0).astype(F32)
            parts += [jnp.where(low_half, lb, 0.0), jnp.where(low_half, 0.0, lb)]
        lm = jnp.concatenate(parts, axis=0).astype(BF16)
        for j in range(TILES):
            wt = jnp.concatenate([recv[s, j * ROWS : (j + 1) * ROWS, :] for s in slots], axis=0)
            o = nt(lhs[j], jnp.concatenate([wt, lm], axis=1))
            for h in range(2):
                cols = pl.ds(pl.multiple_of(firsts[h] * 64, 128), 128)
                if j < 4:
                    merged[pl.ds(starts[j][0], 128), cols] = o[:, 128 * h : 128 * h + 128]
                else:
                    for g in range(4):
                        merged[pl.ds(starts[j][g], 32), cols] = o[32 * g : 32 * g + 32, 128 * h : 128 * h + 128]
            o2 = o * o
            acc[j * 128 : (j + 1) * 128, :] += o2[:, :128] + o2[:, 128:]

    acc[...] = jnp.zeros_like(acc)

    @pl.loop(0, FIRST + len(UNITS))
    def _(s):
        @pl.when(jnp.logical_and(s < 16, inner))
        def _():
            here = place(source(s, 0))
            copy(relay.at[here], relay.at[here], l_send.at[0], l_recv.at[here], mirror).wait_recv()
            relayed(s).start()

        a = s - LAG1

        @pl.when(jnp.logical_and(a >= 0, a < 16))
        def _():
            slot = xl * 32 + source(a, 0)
            arrived(slot)
            forward(slot, a, nbr)
            forward(slot, 16 + a, peer)

        b = s - LAG1 - LAG2

        @pl.when(jnp.logical_and(b >= 0, b < 16))
        def _():
            slot = (1 - xl) * 32 + source(b, 0)
            arrived(slot)
            forward(slot, 32 + b, peer)

        @pl.when(s == 2)
        def _():
            for k in range(1, 8):
                left_copy(lall.at[c, y, (z - k + 8) % 8], k, z_partner(k)).wait_recv()
            for m in left_y:
                m.start()
            for k in range(10, 16):
                send(k)

        @pl.when(s == 7)
        def _():
            for k in range(1, 4):
                left_copy(lall.at[c, (y - k + 4) % 4], 7 + k, y_partner(k)).wait_recv()
            left_core.start()

        @pl.when(s == 8)
        def _():
            left_copy(lall.at[1 - c], 11, (t, peer)).wait_recv()

        @pl.when(s == 3)
        def _():
            pltpu.make_async_copy(rsend, rm, r_recv).wait()

            @pl.when(second)
            def _():
                r_copy(rm, 0).start()

        @pl.when(s == 6)
        def _():
            build_lhs()

        @pl.when(s >= FIRST)
        def _():
            count = 1
            for k, some in enumerate(UNITS):
                count = jnp.where(s == FIRST + k, len(some), count)

            @pl.loop(0, count)
            def _(v):
                w = 0
                for k, some in enumerate(UNITS):
                    for n, u in enumerate(some):
                        w = jnp.where(jnp.logical_and(v == n, s == FIRST + k), u, w)
                unit(w)

    mags = nt(eye, rm[TILES * 16 :, :])
    for j in range(TILES):
        squares = jnp.sum(acc[j * 128 : (j + 1) * 128, :], axis=1, keepdims=True)
        scale = jnp.broadcast_to(mags[:, j : j + 1] / jnp.sqrt(squares + 1e-6), (128, 128))
        for g in range(4):
            scale_ref[pl.ds(starts[j][g], 32), :] = scale[32 * g : 32 * g + 32]

    for m in [left_x, left_core] + left_z + left_y:
        m.wait_send()
    for k in range(16):

        @pl.when(outgoing(k)[2])
        def _():
            copy(send_buf.at[0], relay.at[0], a_send.at[k], l_recv.at[0], mirror).wait_send()

    @pl.loop(0, 16)
    def _(k):
        @pl.when(inner)
        def _():
            relayed(k).wait_send()

    @pl.loop(0, 48)
    def _(k):
        copy(recv.at[0], recv.at[0], f_send.at[k], recv_sem.at[0], (t, peer)).wait_send()

    @pl.when(mine)
    def _():
        for k in range(2):
            r_copy(rsend, k).wait_send()

    @pl.when(second)
    def _():
        r_copy(rm, 0).wait_send()


def scale_kernel(merged, scale, out_hbm, out_ref, sems):
    def written(k):
        rows = pl.ds(k * 32, 32)
        return pltpu.make_async_copy(out_ref.at[rows], out_hbm.at[rows], sems.at[k])

    for k in range(4 * TILES):

        @pl.loop(0, 2)
        def _(n):
            rows = pl.ds(pl.multiple_of(k * 32 + n * 16, 16), 16)
            s = scale[rows, :]
            for i in range(T * ROWS // 128):
                cols = slice(i * 128, i * 128 + 128)
                out_ref[rows, cols] = (merged[rows, cols] * s).astype(BF16)

        written(k).start()
    for k in range(4 * TILES):
        written(k).wait()


def shards(base_weight, adapter_left, adapter_right, magnitude):
    x = base_weight.reshape(EPS, ROWS, 3584)
    left = jnp.swapaxes(adapter_left, 2, 3).reshape(EPS, 16, ROWS)
    right = adapter_right.reshape(EPS, 16, 3584)
    x, left, right, magnitude = (pltpu.with_memory_space_constraint(a, pltpu.HBM) for a in (x, left, right, magnitude))
    vmem = pl.BlockSpec(memory_space=pltpu.VMEM)
    merged, scale = pl.pallas_call(
        exchange_kernel,
        out_shape=(pltpu.VMEM((EPS * SERVE, T * ROWS), F32), pltpu.VMEM((EPS * SERVE, 128), F32)),
        in_specs=[pl.BlockSpec(memory_space=pltpu.HBM)] * 4,
        out_specs=(vmem, vmem),
        scratch_shapes=[
            pltpu.VMEM((EPS, ROWS, 3584), BF16),
            pltpu.VMEM((EPS, 16, ROWS), BF16),
            pltpu.VMEM((EPS, 16, 3584), BF16),
            pltpu.VMEM((2, 2, 3584), BF16),
            pltpu.SemaphoreType.DMA((7,)),
            pltpu.VMEM((16, WROWS, 128), BF16),
            pltpu.VMEM((RROWS, 128), BF16),
            pltpu.VMEM((T, WROWS, 128), BF16),
            pltpu.VMEM((16, WROWS, 128), BF16),
            pltpu.VMEM((RROWS, 128), BF16),
            pltpu.VMEM((EPS * SERVE, 128), F32),
            pltpu.VMEM((TILES, 128, 256), BF16),
            pltpu.VMEM((2, 4, 8, 2, LROWS // 2, 128), BF16),
            pltpu.SemaphoreType.DMA((16,)),
            pltpu.SemaphoreType.DMA((16,)),
            pltpu.SemaphoreType.DMA((48,)),
            pltpu.SemaphoreType.DMA((2,)),
            pltpu.SemaphoreType.DMA((T,)),
            pltpu.SemaphoreType.DMA((16,)),
            pltpu.SemaphoreType.DMA,
            pltpu.SemaphoreType.DMA((12,)),
            pltpu.SemaphoreType.DMA((12,)),
        ],
        compiler_params=pltpu.CompilerParams(collective_id=0, has_side_effects=True, vmem_limit_bytes=24 * 2**20),
        name="exchange",
    )(x, left, right, magnitude)
    out = pl.pallas_call(
        scale_kernel,
        out_shape=jax.ShapeDtypeStruct((EPS * SERVE, T * ROWS), BF16),
        in_specs=[vmem, vmem],
        out_specs=pl.BlockSpec(memory_space=pltpu.HBM),
        scratch_shapes=[pltpu.VMEM((EPS * SERVE, T * ROWS), BF16), pltpu.SemaphoreType.DMA((4 * TILES,))],
        compiler_params=pltpu.CompilerParams(vmem_limit_bytes=16 * 2**20),
        name="scale",
    )(merged, scale)
    return out.reshape(2, 2, SERVE, T * ROWS)


def solution(mesh):
    in_specs = (
        P(None, None, "tensor", "dp"),
        P(None, None, "tensor", None),
        P(None, None, None, "dp"),
        P(None, None, "dp"),
    )
    out_specs = P(None, None, "tensor", None)
    return jax.shard_map(shards, mesh=mesh, in_specs=in_specs, out_specs=out_specs, check_vma=False)
```

```python
import functools

import jax
import jax.numpy as jnp
from jax import lax
from jax.experimental import pallas as pl
from jax.experimental.pallas import tpu as pltpu
from jax.sharding import PartitionSpec as P

MESH = pl.DeviceIdType.MESH
F32, BF16 = jnp.float32, jnp.bfloat16

T = 64
ROWS = 64
SERVE = 224
EPS = 4
TILES = 7
WROWS = TILES * ROWS
LROWS = 32
RROWS = TILES * 16 + 16
LAG1, LAG2 = 2, 3
FIRST = 10
UNITS = ((0,), (1,), (4,), (2,), (5,), (3,), (8,), (6,), (9, 7), (12, 10, 11), (13, 14), (15,))


def packed(load, m):
    hole = 3 - m
    full = [load(e, 2 * m) for e in range(EPS)]
    rest = []
    for e in range(EPS):
        if m == 0:
            rest.append(load(e, 1))
        elif m == 3:
            rest.append(load(e, 5))
        else:
            low, high = load(e, 2 * m + 1), load(e, 2 * m - 1)
            group = lax.broadcasted_iota(jnp.int32, low.shape, 1) // 32
            rest.append(jnp.where(group < hole, low, high))
    last = rest[3].astype(F32)
    group = lax.broadcasted_iota(jnp.int32, last.shape, 1) // 32
    for k in range(3):
        full.append(jnp.where(group == hole, pltpu.roll(last, 32 * (k + 1), 1).astype(BF16), rest[k]))
    return full


def nt(a, b):
    return lax.dot_general(a, b, (((1,), (1,)), ((), ())), preferred_element_type=F32)


SENDS = tuple((d, p) for d in (0, 1, -1, 2, -2, 3, -3, 4) for p in (0, 1))


def arrival(s):
    even = lax.rem(s, 2) == 0
    far = jnp.where(s >= 10, 3, 2)
    dz_near = jnp.where(jnp.logical_or(s == 0, s == 5), 0, jnp.where(even, -1, 1))
    dz_far = jnp.where(s >= 14, 4, jnp.where(even, far, -far))
    late = jnp.where(s < 6, s >= 3, jnp.where(s < 10, s >= 8, jnp.where(s < 14, s >= 12, s == 15)))
    return jnp.where(s < 6, dz_near, dz_far), late


def exchange_kernel(
    x_hbm, l_hbm, r_hbm, m_hbm, merged, scale_ref, x_ref, l_ref, r_ref, m_ref, in_sem, send_buf, rsend, recv, relay, rm, acc, lhs, lall, a_send, l_send, f_send, r_send, recv_sem, l_recv, r_recv, g_send, g_recv
):
    t, q = lax.axis_index("tensor"), lax.axis_index("dp")
    xh, y, z = t // 32, (t // 8) % 4, t % 8
    xl, c = q // 2, q % 2
    nbr, peer = q + 2 - 4 * xl, q + 1 - 2 * c
    edge, inner = xh == xl, xh != xl
    mirror = (xl * 32 + y * 8 + z, 2 * xh + c)
    src_core, dst_core = y // 2, y % 2
    row_m = t % 4
    hole = 3 - row_m

    y_rows = [[(y + (y + parity) % 2 + 2 * w) % 4 * 8 for w in range(2)] for parity in (c, 1 - c)]

    def source(s, who):
        dz, late = arrival(s)
        return jnp.where(late, y_rows[who][1], y_rows[who][0]) + lax.rem(z - dz + 8, 8)

    def place(yz):
        return lax.div(yz, 16) * 8 + lax.rem(yz, 8)

    small_in = [pltpu.make_async_copy(a, b, in_sem.at[4 + k]) for k, (a, b) in enumerate(((l_hbm, l_ref), (r_hbm, r_ref), (m_hbm, m_ref)))]

    def x_in(g):
        cols = pl.ds(pl.multiple_of(g * (TILES * 128), 128), TILES * 128)
        return pltpu.make_async_copy(x_hbm.at[:, :, cols], x_ref.at[:, :, cols], in_sem.at[g])


    barrier = pltpu.get_barrier_semaphore()

    for n in range(16):
        yz = source(15 - n, 0)

        @pl.when(jnp.logical_or(yz != y * 8 + z, src_core != c))
        def _():
            pl.semaphore_signal(barrier, inc=1, device_id=(xh * 32 + yz, xl * 2 + src_core), device_id_type=MESH)

    opposite = ((1 - xh) * 32 + y * 8 + z, (1 - xl) * 2 + c)

    def z_partner(k):
        return (xh * 32 + y * 8 + (z + k) % 8, q)

    def y_partner(k):
        return (xh * 32 + (y + k) % 4 * 8 + z, q)

    greeted = [z_partner(k) for k in (4, 3, 5, 2, 6, 1, 7)] + [(t, nbr), (t, peer), opposite] + [y_partner(k) for k in range(1, 4)]
    for other in greeted:
        pl.semaphore_signal(barrier, inc=1, device_id=other, device_id_type=MESH)

    for a in small_in:
        a.start()
    for g in range(4):
        x_in(g).start()

    for a in small_in:
        a.wait()
    lanes = lax.broadcasted_iota(jnp.int32, (16, 128), 1)
    ranks = lax.broadcasted_iota(jnp.int32, (16, 128), 0)
    lpack = jnp.zeros((LROWS, 128), F32)
    for e in range(EPS):
        low = (lanes == e * 16 + ranks).astype(BF16)
        high = (lanes == 64 + e * 16 + ranks).astype(BF16)
        tn = functools.partial(lax.dot_general, dimension_numbers=(((0,), (0,)), ((), ())), preferred_element_type=F32)
        lpack += tn(l_ref[e], low)[:LROWS] + tn(l_ref[e], high)[LROWS:]
    lall[c, y, z, xh] = jnp.where(c == 0, lpack[:16], lpack[16:]).astype(BF16)

    @pl.loop(0, 4)
    def _(g):
        base = g * (TILES * 128)
        x_in(g).wait()

        def at(k):
            return pl.ds(pl.multiple_of(base + 128 * k, 128), 128)

        for m in range(4):
            d = g * 4 + m
            for j, tile in enumerate(packed(lambda e, k: x_ref[e, :, at(k)], m)):
                send_buf[d, j * ROWS : (j + 1) * ROWS, :] = tile

    mine = q == t // 16
    for m in range(4):

        @pl.when(jnp.logical_and(mine, row_m == m))
        def _():
            base = t % 16 // 4 * (TILES * 128)

            def at(k):
                return pl.ds(pl.multiple_of(base + 128 * k, 128), 128)

            rt = packed(lambda e, k: r_ref[e, :, at(k)], m)
            mt = packed(lambda e, k: jnp.broadcast_to(m_ref[e // 2, :, at(k)].astype(F32)[e % 2 : e % 2 + 1], (16, 128)).astype(BF16), m)
            mags = jnp.zeros((16, 128), F32)
            for j in range(TILES):
                rsend[j * 16 : j * 16 + 16, :] = rt[j]
                mags = jnp.where(ranks == j, mt[j].astype(F32), mags)
            rsend[TILES * 16 :, :] = mags.astype(BF16)

    self_out = jnp.logical_and(src_core == c, dst_core == c).astype(jnp.int32)
    pl.semaphore_wait(barrier, 16 + len(greeted) - self_out)

    def copy(src, dst, send, recv_s, dev):
        return pltpu.make_async_remote_copy(
            src_ref=src, dst_ref=dst, send_sem=send, recv_sem=recv_s, device_id=dev, device_id_type=MESH
        )

    second = nbr == t // 16

    def r_copy(src, k):
        return copy(src, rm, r_send.at[k], r_recv, (t, (peer, nbr)[k]))

    @pl.when(mine)
    def _():
        for k in range(2):
            r_copy(rsend, k).start()
        pltpu.make_async_copy(rsend, rm, r_recv).start()

    def outgoing(k):
        dz, p = SENDS[k]
        yd, zd = 2 * c + (y + p) % 2, (z + dz + 8) % 8
        away = jnp.logical_or(jnp.logical_or(yd != y, zd != z), dst_core != c)
        return yd, zd, away

    own = place(y * 8 + z)

    def send(k):
        yd, zd, away = outgoing(k)
        dev = (xh * 32 + yd * 8 + zd, xl * 2 + dst_core)
        block = send_buf.at[(yd - 2 * c) * 8 + zd]

        @pl.when(jnp.logical_and(away, edge))
        def _():
            copy(block, recv.at[t], a_send.at[k], recv_sem.at[t], dev).start()

        @pl.when(jnp.logical_and(away, inner))
        def _():
            copy(block, relay.at[own], a_send.at[k], l_recv.at[own], dev).start()

        @pl.when(jnp.logical_and(jnp.logical_not(away), edge))
        def _():
            pltpu.make_async_copy(block, recv.at[t], recv_sem.at[t]).start()

        @pl.when(jnp.logical_and(jnp.logical_not(away), inner))
        def _():
            pltpu.make_async_copy(block, relay.at[own], l_recv.at[own]).start()

    def left_copy(ref, k, dev):
        return copy(ref, ref, g_send.at[k], g_recv.at[k], dev)

    left_x = left_copy(lall.at[c, y, z, xh], 0, opposite)
    left_z = [left_copy(lall.at[c, y, z], k, z_partner(k)) for k in range(1, 8)]
    left_y = [left_copy(lall.at[c, y], 7 + k, y_partner(k)) for k in range(1, 4)]
    left_core = left_copy(lall.at[c], 11, (t, peer))

    left_x.start()
    for k in range(6):
        send(k)
    left_copy(lall.at[c, y, z, 1 - xh], 0, opposite).wait_recv()
    for m in left_z:
        m.start()
    for k in range(6, 16):
        send(k)

    def arrived(slot):
        copy(recv.at[slot], recv.at[slot], f_send.at[0], recv_sem.at[slot], (t, peer)).wait_recv()

    def forward(slot, k, other):
        copy(recv.at[slot], recv.at[slot], f_send.at[k], recv_sem.at[slot], (t, other)).start()

    def relayed(s):
        yz = source(s, 0)
        slot = xh * 32 + yz
        return copy(relay.at[place(yz)], recv.at[slot], l_send.at[s], recv_sem.at[slot], mirror)

    lane = lax.broadcasted_iota(jnp.int32, (128, 128), 1)
    row = lax.broadcasted_iota(jnp.int32, (128, 128), 0)
    eye = (lane == row).astype(BF16)

    def build_lhs():
        for j in range(TILES):
            r = rm[j * 16 : j * 16 + 16, :].astype(F32)
            r8 = jnp.concatenate([r] * 8, axis=0)
            e_lane = j if j < 4 else jnp.where(lane // 32 == hole, 3, j - 4)
            rbd = jnp.where((row // 16) % 4 == e_lane, r8, 0.0).astype(BF16)
            lhs[j, :, 0:128] = eye
            lhs[j, :, 128:256] = nt(eye, rbd).astype(BF16)

    def column(g):
        return jnp.where(g > hole, 32 * (g - hole - 1), 128 + 32 * row_m + 32 * g)

    def row_start(j, g):
        if j < 4:
            return pl.multiple_of(SERVE * j + 32 * row_m + 32 * g, 32)
        k = j - 4
        from3 = (hole - k - 1 + 4) % 4
        return pl.multiple_of(jnp.where(hole == g, SERVE * 3 + column(from3), SERVE * k + column(g)), 32)

    starts = [[row_start(j, g) for g in range(4)] for j in range(TILES)]
    low_half = lax.broadcasted_iota(jnp.int32, (LROWS, 128), 1) < 64

    def unit(w):
        stage, who = w // 4, w % 4
        half = jnp.where(who % 2 == 1, 1 - xl, xl)
        parity = jnp.where(who >= 2, 1 - c, c)
        odd = z % 2
        step = jnp.where(stage == 0, 0, jnp.where(stage == 1, -2, jnp.where(stage == 2, 2, 4)))
        zp = (z - odd + (1 - 2 * odd) * step + 8) % 8
        firsts = [half * 32 + (parity + 2 * h) * 8 + zp for h in range(2)]
        slots = [f + k for f in firsts for k in range(2)]

        @pl.when(who >= 2)
        def _():
            @pl.loop(jnp.where(stage == 0, 0, 2 + 4 * stage), jnp.where(stage == 3, 16, 6 + 4 * stage))
            def _(i):
                arrived(half * 32 + source(i, 1))

        parts = []
        for h, k in ((0, 0), (0, 1), (1, 0), (1, 1)):
            lb = jnp.concatenate([lall[n, parity + 2 * h, zp + k, half] for n in range(2)], axis=0).astype(F32)
            parts += [jnp.where(low_half, lb, 0.0), jnp.where(low_half, 0.0, lb)]
        lm = jnp.concatenate(parts, axis=0).astype(BF16)
        for j in range(TILES):
            wt = jnp.concatenate([recv[s, j * ROWS : (j + 1) * ROWS, :] for s in slots], axis=0)
            o = nt(lhs[j], jnp.concatenate([wt, lm], axis=1))
            for h in range(2):
                cols = pl.ds(pl.multiple_of(firsts[h] * 64, 128), 128)
                if j < 4:
                    merged[pl.ds(starts[j][0], 128), cols] = o[:, 128 * h : 128 * h + 128]
                else:
                    for g in range(4):
                        merged[pl.ds(starts[j][g], 32), cols] = o[32 * g : 32 * g + 32, 128 * h : 128 * h + 128]
            o2 = o * o
            acc[j * 128 : (j + 1) * 128, :] += o2[:, :128] + o2[:, 128:]

    acc[...] = jnp.zeros_like(acc)

    @pl.loop(0, FIRST + len(UNITS))
    def _(s):
        @pl.when(jnp.logical_and(s < 16, inner))
        def _():
            here = place(source(s, 0))
            copy(relay.at[here], relay.at[here], l_send.at[0], l_recv.at[here], mirror).wait_recv()
            relayed(s).start()

        a = s - LAG1

        @pl.when(jnp.logical_and(a >= 0, a < 16))
        def _():
            slot = xl * 32 + source(a, 0)
            arrived(slot)
            forward(slot, a, nbr)
            forward(slot, 16 + a, peer)

        b = s - LAG1 - LAG2

        @pl.when(jnp.logical_and(b >= 0, b < 16))
        def _():
            slot = (1 - xl) * 32 + source(b, 0)
            arrived(slot)
            forward(slot, 32 + b, peer)

        @pl.when(s == 3)
        def _():
            for k in range(1, 8):
                left_copy(lall.at[c, y, (z - k + 8) % 8], k, z_partner(k)).wait_recv()
            for m in left_y:
                m.start()

        @pl.when(s == 7)
        def _():
            for k in range(1, 4):
                left_copy(lall.at[c, (y - k + 4) % 4], 7 + k, y_partner(k)).wait_recv()
            left_core.start()

        @pl.when(s == 8)
        def _():
            left_copy(lall.at[1 - c], 11, (t, peer)).wait_recv()

        @pl.when(s == 3)
        def _():
            pltpu.make_async_copy(rsend, rm, r_recv).wait()

            @pl.when(second)
            def _():
                r_copy(rm, 0).start()

        @pl.when(s == 6)
        def _():
            build_lhs()

        @pl.when(s >= FIRST)
        def _():
            count = 1
            for k, some in enumerate(UNITS):
                count = jnp.where(s == FIRST + k, len(some), count)

            @pl.loop(0, count)
            def _(v):
                w = 0
                for k, some in enumerate(UNITS):
                    for n, u in enumerate(some):
                        w = jnp.where(jnp.logical_and(v == n, s == FIRST + k), u, w)
                unit(w)

    mags = nt(eye, rm[TILES * 16 :, :])
    for j in range(TILES):
        squares = jnp.sum(acc[j * 128 : (j + 1) * 128, :], axis=1, keepdims=True)
        scale = jnp.broadcast_to(mags[:, j : j + 1] / jnp.sqrt(squares + 1e-6), (128, 128))
        for g in range(4):
            scale_ref[pl.ds(starts[j][g], 32), :] = scale[32 * g : 32 * g + 32]

    for m in [left_x, left_core] + left_z + left_y:
        m.wait_send()
    for k in range(16):

        @pl.when(outgoing(k)[2])
        def _():
            copy(send_buf.at[0], relay.at[0], a_send.at[k], l_recv.at[0], mirror).wait_send()

    @pl.loop(0, 16)
    def _(k):
        @pl.when(inner)
        def _():
            relayed(k).wait_send()

    @pl.loop(0, 48)
    def _(k):
        copy(recv.at[0], recv.at[0], f_send.at[k], recv_sem.at[0], (t, peer)).wait_send()

    @pl.when(mine)
    def _():
        for k in range(2):
            r_copy(rsend, k).wait_send()

    @pl.when(second)
    def _():
        r_copy(rm, 0).wait_send()


def scale_kernel(merged, scale, out_hbm, out_ref, sems):
    def written(k):
        rows = pl.ds(k * 32, 32)
        return pltpu.make_async_copy(out_ref.at[rows], out_hbm.at[rows], sems.at[k])

    for k in range(4 * TILES):

        @pl.loop(0, 2)
        def _(n):
            rows = pl.ds(pl.multiple_of(k * 32 + n * 16, 16), 16)
            s = scale[rows, :]
            for i in range(T * ROWS // 128):
                cols = slice(i * 128, i * 128 + 128)
                out_ref[rows, cols] = (merged[rows, cols] * s).astype(BF16)

        written(k).start()
    for k in range(4 * TILES):
        written(k).wait()


def shards(base_weight, adapter_left, adapter_right, magnitude):
    x = base_weight.reshape(EPS, ROWS, 3584)
    left = jnp.swapaxes(adapter_left, 2, 3).reshape(EPS, 16, ROWS)
    right = adapter_right.reshape(EPS, 16, 3584)
    x, left, right, magnitude = (pltpu.with_memory_space_constraint(a, pltpu.HBM) for a in (x, left, right, magnitude))
    vmem = pl.BlockSpec(memory_space=pltpu.VMEM)
    merged, scale = pl.pallas_call(
        exchange_kernel,
        out_shape=(pltpu.VMEM((EPS * SERVE, T * ROWS), F32), pltpu.VMEM((EPS * SERVE, 128), F32)),
        in_specs=[pl.BlockSpec(memory_space=pltpu.HBM)] * 4,
        out_specs=(vmem, vmem),
        scratch_shapes=[
            pltpu.VMEM((EPS, ROWS, 3584), BF16),
            pltpu.VMEM((EPS, 16, ROWS), BF16),
            pltpu.VMEM((EPS, 16, 3584), BF16),
            pltpu.VMEM((2, 2, 3584), BF16),
            pltpu.SemaphoreType.DMA((7,)),
            pltpu.VMEM((16, WROWS, 128), BF16),
            pltpu.VMEM((RROWS, 128), BF16),
            pltpu.VMEM((T, WROWS, 128), BF16),
            pltpu.VMEM((16, WROWS, 128), BF16),
            pltpu.VMEM((RROWS, 128), BF16),
            pltpu.VMEM((EPS * SERVE, 128), F32),
            pltpu.VMEM((TILES, 128, 256), BF16),
            pltpu.VMEM((2, 4, 8, 2, LROWS // 2, 128), BF16),
            pltpu.SemaphoreType.DMA((16,)),
            pltpu.SemaphoreType.DMA((16,)),
            pltpu.SemaphoreType.DMA((48,)),
            pltpu.SemaphoreType.DMA((2,)),
            pltpu.SemaphoreType.DMA((T,)),
            pltpu.SemaphoreType.DMA((16,)),
            pltpu.SemaphoreType.DMA,
            pltpu.SemaphoreType.DMA((12,)),
            pltpu.SemaphoreType.DMA((12,)),
        ],
        compiler_params=pltpu.CompilerParams(collective_id=0, has_side_effects=True, vmem_limit_bytes=24 * 2**20),
        name="exchange",
    )(x, left, right, magnitude)
    out = pl.pallas_call(
        scale_kernel,
        out_shape=jax.ShapeDtypeStruct((EPS * SERVE, T * ROWS), BF16),
        in_specs=[vmem, vmem],
        out_specs=pl.BlockSpec(memory_space=pltpu.HBM),
        scratch_shapes=[pltpu.VMEM((EPS * SERVE, T * ROWS), BF16), pltpu.SemaphoreType.DMA((4 * TILES,))],
        compiler_params=pltpu.CompilerParams(vmem_limit_bytes=16 * 2**20),
        name="scale",
    )(merged, scale)
    return out.reshape(2, 2, SERVE, T * ROWS)


def solution(mesh):
    in_specs = (
        P(None, None, "tensor", "dp"),
        P(None, None, "tensor", None),
        P(None, None, None, "dp"),
        P(None, None, "dp"),
    )
    out_specs = P(None, None, "tensor", None)
    return jax.shard_map(shards, mesh=mesh, in_specs=in_specs, out_specs=out_specs, check_vma=False)
```
